64 devices in a mesh: rep: 4 (over x, y), dp: 16 (over z, core).
Axes of the slice: x: 2, y: 2, z: 8, core: 2. Of those that a mesh axis runs over, the one named last changes fastest.
The devices are a block of a 4x4x8 slice.
Arguments:
- hidden: bfloat16 [2048, 2048], P(('rep', 'dp')), parts along dimension 0
- ckv_cache: bfloat16 [2048, 128, 512], P(('rep', 'dp')), parts along dimension 0
- kr_cache: bfloat16 [2048, 128, 64], P(('rep', 'dp')), parts along dimension 0
- seq_lens: int32 [2048], P(('rep', 'dp')), parts along dimension 0
- expert_ids: int32 [2048, 6], P(('rep', 'dp')), parts along dimension 0
- attn_gain: bfloat16 [2048], replicated
- kv_gain: bfloat16 [512], replicated
- moe_gain: bfloat16 [2048], replicated
- w_q: bfloat16 [2048, 3072], replicated
- w_dkv: bfloat16 [2048, 576], replicated
- w_uk: bfloat16 [16, 128, 512], replicated
- w_uv: bfloat16 [16, 512, 128], replicated
- w_o: bfloat16 [2048, 2048], replicated
- w_router: bfloat16 [2048, 64], replicated
- shared_gate: bfloat16 [2048, 2816], replicated
- shared_up: bfloat16 [2048, 2816], replicated
- shared_down: bfloat16 [2816, 2048], replicated
- expert_gate: bfloat16 [64, 2048, 1408], P('dp')
- expert_up: bfloat16 [64, 2048, 1408], P('dp')
- expert_down: bfloat16 [64, 1408, 2048], P('dp')
Outputs:
- output 1: bfloat16 [2048, 2048], P(('rep', 'dp')), parts along dimension 0
- output 2: bfloat16 [2048, 512], P(('rep', 'dp')), parts along dimension 0
- output 3: bfloat16 [2048, 64], P(('rep', 'dp')), parts along dimension 0
There are 4 independent parts. The reference program is written for one: setup_inputs(seed, part) draws one part's arguments, and reference() takes and returns one part's arrays. A program takes and returns all parts, laid end to end along the dimension named above; an argument that names none is the same for every part.
All inputs are finite; a program needn't handle non-finite values.
Results may differ from the reference program's by a relative error of at most 0.0123531.
Values are sent between devices in bfloat16 or wider.
A program may use at most 768 MiB of HBM per device.

```python
import jax
import jax.numpy as jnp
from jax import lax

DP_SIZE = 16
SEQS_DEV = 32
CACHE_LEN = 128
D_MODEL = 2048
HEADS = 16
NOPE_DIM = 128
ROPE_DIM = 64
V_DIM = 128
KV_LORA = 512
EXPERTS = 64
TOP_K = 6
FF_DIM = 1408
N_SHARED = 2

GROUP_ROWS = DP_SIZE * SEQS_DEV
SLOT_CAP = max(2, (2 * SEQS_DEV * TOP_K) // EXPERTS)
NORM_EPS = 1e-6
ROPE_THETA = 10000.0
SCORE_SCALE = (NOPE_DIM + ROPE_DIM) ** -0.5


def normal_bf16(draw_key, arr_shape, std_scale):
    return (jax.random.normal(draw_key, arr_shape, jnp.float32) * std_scale).astype(jnp.bfloat16)


def draw_gain(draw_key, gain_len):
    return jax.random.uniform(draw_key, (gain_len,), jnp.float32, minval=0.5, maxval=1.5).astype(jnp.bfloat16)


def draw_lengths(len_key):
    base_key, order_key = jax.random.split(len_key)
    base_lens = jax.random.randint(base_key, (GROUP_ROWS,), CACHE_LEN // 8, CACHE_LEN)
    seq_order = jax.random.permutation(order_key, GROUP_ROWS)
    return base_lens.at[seq_order[0]].set(CACHE_LEN - 1).at[seq_order[1]].set(CACHE_LEN // 8).astype(jnp.int32)


def draw_routes(route_key):
    hot_key, dev_key = jax.random.split(route_key)
    hot_expert = jax.random.randint(hot_key, (), 0, EXPERTS)
    choice_col = jnp.arange(TOP_K)

    def one_device(device_key):
        perm_key, rank_key = jax.random.split(device_key)
        other_ids = jax.random.permutation(perm_key, EXPERTS - 1)
        other_ids = other_ids + (other_ids >= hot_expert).astype(other_ids.dtype)
        tok_rank = jax.random.permutation(rank_key, SEQS_DEV)
        cycle_pos = (tok_rank[:, None] * TOP_K + choice_col[None, :]) % (EXPERTS - 1)
        is_hot = (tok_rank[:, None] < SLOT_CAP) & (choice_col[None, :] == 0)
        return jnp.where(is_hot, hot_expert, other_ids[cycle_pos])

    routes = jax.vmap(one_device)(jax.random.split(dev_key, DP_SIZE))
    return routes.reshape(GROUP_ROWS, TOP_K).astype(jnp.int32)


def setup_inputs(seed: int = 0, part: int = 0) -> dict:
    root_key = jax.random.key(seed)
    part_keys = jax.random.split(jax.random.fold_in(root_key, part), 5)
    weight_keys = jax.random.split(root_key, 15)
    return {
        'hidden': normal_bf16(part_keys[0], (GROUP_ROWS, D_MODEL), 1.0),
        'ckv_cache': normal_bf16(part_keys[1], (GROUP_ROWS, CACHE_LEN, KV_LORA), 1.0),
        'kr_cache': normal_bf16(part_keys[2], (GROUP_ROWS, CACHE_LEN, ROPE_DIM), 1.0),
        'seq_lens': draw_lengths(part_keys[3]),
        'expert_ids': draw_routes(part_keys[4]),
        'attn_gain': draw_gain(weight_keys[0], D_MODEL),
        'kv_gain': draw_gain(weight_keys[1], KV_LORA),
        'moe_gain': draw_gain(weight_keys[2], D_MODEL),
        'w_q': normal_bf16(weight_keys[3], (D_MODEL, HEADS * (NOPE_DIM + ROPE_DIM)), D_MODEL ** -0.5),
        'w_dkv': normal_bf16(weight_keys[4], (D_MODEL, KV_LORA + ROPE_DIM), D_MODEL ** -0.5),
        'w_uk': normal_bf16(weight_keys[5], (HEADS, NOPE_DIM, KV_LORA), NOPE_DIM ** -0.5),
        'w_uv': normal_bf16(weight_keys[6], (HEADS, KV_LORA, V_DIM), 2.0 * KV_LORA ** -0.5),
        'w_o': normal_bf16(weight_keys[7], (HEADS * V_DIM, D_MODEL), 2.0 * (HEADS * V_DIM) ** -0.5),
        'w_router': normal_bf16(weight_keys[8], (D_MODEL, EXPERTS), D_MODEL ** -0.5),
        'shared_gate': normal_bf16(weight_keys[9], (D_MODEL, N_SHARED * FF_DIM), D_MODEL ** -0.5),
        'shared_up': normal_bf16(weight_keys[10], (D_MODEL, N_SHARED * FF_DIM), D_MODEL ** -0.5),
        'shared_down': normal_bf16(weight_keys[11], (N_SHARED * FF_DIM, D_MODEL), (N_SHARED * FF_DIM) ** -0.5),
        'expert_gate': normal_bf16(weight_keys[12], (EXPERTS, D_MODEL, FF_DIM), D_MODEL ** -0.5),
        'expert_up': normal_bf16(weight_keys[13], (EXPERTS, D_MODEL, FF_DIM), D_MODEL ** -0.5),
        'expert_down': normal_bf16(weight_keys[14], (EXPERTS, FF_DIM, D_MODEL), 2.0 * EXPERTS / TOP_K * FF_DIM ** -0.5),
    }


def rms_norm(values, gain_vec):
    vals_f32 = values.astype(jnp.float32)
    inv_rms = lax.rsqrt(jnp.mean(vals_f32 * vals_f32, axis=-1, keepdims=True) + NORM_EPS)
    return (vals_f32 * inv_rms * gain_vec.astype(jnp.float32)).astype(jnp.bfloat16)


def rope_tables(positions):
    inv_freq = ROPE_THETA ** (-2.0 * jnp.arange(ROPE_DIM // 2, dtype=jnp.float32) / ROPE_DIM)
    angles = positions.astype(jnp.float32)[:, None] * inv_freq[None, :]
    return jnp.cos(angles), jnp.sin(angles)


def apply_rope(values, rope_cos, rope_sin):
    half_dim = values.shape[-1] // 2
    first_half = values[..., :half_dim]
    second_half = values[..., half_dim:]
    return jnp.concatenate([first_half * rope_cos - second_half * rope_sin, second_half * rope_cos + first_half * rope_sin], axis=-1)


def attend_one(row_args):
    q_lat_row, q_rot_row, ckv_row, kr_row, seq_len, ckv_new_row, kr_new_row = row_args
    q_lat_f32 = q_lat_row.astype(jnp.float32)
    q_rot_f32 = q_rot_row.astype(jnp.float32)
    ckv_f32 = ckv_row.astype(jnp.float32)
    kr_f32 = kr_row.astype(jnp.float32)
    ckv_new_f32 = ckv_new_row.astype(jnp.float32)
    kr_new_f32 = kr_new_row.astype(jnp.float32)
    scores = (jnp.dot(q_lat_f32, ckv_f32.T) + jnp.dot(q_rot_f32, kr_f32.T)) * SCORE_SCALE
    valid_mask = jnp.arange(CACHE_LEN) < seq_len
    scores = jnp.where(valid_mask[None, :], scores, -jnp.inf)
    new_score = (jnp.dot(q_lat_f32, ckv_new_f32) + jnp.dot(q_rot_f32, kr_new_f32)) * SCORE_SCALE
    top_score = jnp.maximum(jnp.max(scores, axis=-1), new_score)
    exp_cache = jnp.exp(scores - top_score[:, None])
    exp_new = jnp.exp(new_score - top_score)
    denominator = jnp.sum(exp_cache, axis=-1) + exp_new
    prob_cache = (exp_cache / denominator[:, None]).astype(jnp.bfloat16).astype(jnp.float32)
    prob_new = (exp_new / denominator).astype(jnp.bfloat16).astype(jnp.float32)
    o_lat = jnp.dot(prob_cache, ckv_f32) + prob_new[:, None] * ckv_new_f32[None, :]
    return o_lat.astype(jnp.bfloat16)


def routed_experts(moe_in, gate_vals, expert_ids, expert_gate, expert_up, expert_down):
    rows_max = DP_SIZE * SLOT_CAP
    pad_in = jnp.concatenate([moe_in, jnp.zeros((1, D_MODEL), moe_in.dtype)], axis=0)

    def per_expert(acc_out, expert_no):
        picked = expert_ids == expert_no
        gate_tok = jnp.concatenate([jnp.sum(jnp.where(picked, gate_vals, 0.0), axis=-1), jnp.zeros((1,), gate_vals.dtype)])
        row_ids = jnp.nonzero(jnp.any(picked, axis=-1), size=rows_max, fill_value=GROUP_ROWS)[0]
        tok_rows = pad_in[row_ids]
        gate_act = jnp.dot(tok_rows, expert_gate[expert_no], preferred_element_type=jnp.float32)
        up_act = jnp.dot(tok_rows, expert_up[expert_no], preferred_element_type=jnp.float32)
        mid_act = (jax.nn.silu(gate_act) * up_act).astype(jnp.bfloat16)
        expert_out = jnp.dot(mid_act, expert_down[expert_no], preferred_element_type=jnp.float32).astype(jnp.bfloat16)
        acc_out = acc_out.at[row_ids].add(gate_tok[row_ids][:, None] * expert_out.astype(jnp.float32), mode='drop')
        return acc_out, None

    scanned = lax.scan(per_expert, jnp.zeros((GROUP_ROWS, D_MODEL), jnp.float32), jnp.arange(EXPERTS))
    return scanned[0]


def reference(hidden, ckv_cache, kr_cache, seq_lens, expert_ids, attn_gain, kv_gain, moe_gain, w_q, w_dkv, w_uk, w_uv, w_o, w_router, shared_gate, shared_up, shared_down, expert_gate, expert_up, expert_down):
    normed_x = rms_norm(hidden, attn_gain)
    q_all = jnp.dot(normed_x, w_q, preferred_element_type=jnp.float32).astype(jnp.bfloat16).reshape(GROUP_ROWS, HEADS, NOPE_DIM + ROPE_DIM)
    latent_kv = jnp.dot(normed_x, w_dkv, preferred_element_type=jnp.float32)
    ckv_new = rms_norm(latent_kv[:, :KV_LORA], kv_gain)
    rope_cos, rope_sin = rope_tables(seq_lens)
    kr_new = apply_rope(latent_kv[:, KV_LORA:], rope_cos, rope_sin).astype(jnp.bfloat16)
    q_rot = apply_rope(q_all[:, :, NOPE_DIM:].astype(jnp.float32), rope_cos[:, None, :], rope_sin[:, None, :]).astype(jnp.bfloat16)
    q_lat = jnp.einsum('bhn,hnc->bhc', q_all[:, :, :NOPE_DIM].astype(jnp.float32), w_uk.astype(jnp.float32)).astype(jnp.bfloat16)
    o_lat = lax.map(attend_one, (q_lat, q_rot, ckv_cache, kr_cache, seq_lens, ckv_new, kr_new))
    head_out = jnp.einsum('bhc,hcv->bhv', o_lat.astype(jnp.float32), w_uv.astype(jnp.float32)).astype(jnp.bfloat16).reshape(GROUP_ROWS, HEADS * V_DIM)
    resid_out = (hidden.astype(jnp.float32) + jnp.dot(head_out, w_o, preferred_element_type=jnp.float32)).astype(jnp.bfloat16)
    moe_in = rms_norm(resid_out, moe_gain)
    router_prob = jax.nn.softmax(jnp.dot(moe_in, w_router, preferred_element_type=jnp.float32), axis=-1)
    gate_vals = jnp.take_along_axis(router_prob, expert_ids, axis=-1)
    shared_act = (jax.nn.silu(jnp.dot(moe_in, shared_gate, preferred_element_type=jnp.float32)) * jnp.dot(moe_in, shared_up, preferred_element_type=jnp.float32)).astype(jnp.bfloat16)
    shared_out = jnp.dot(shared_act, shared_down, preferred_element_type=jnp.float32)
    routed_out = routed_experts(moe_in, gate_vals, expert_ids, expert_gate, expert_up, expert_down)
    layer_out = (resid_out.astype(jnp.float32) + shared_out + routed_out).astype(jnp.bfloat16)
    return layer_out, ckv_new, kr_new
```

```python
import functools

import jax
import jax.numpy as jnp
from jax import lax
from jax.experimental import pallas as pl
from jax.experimental.pallas import tpu as pltpu
from jax.sharding import PartitionSpec as P

NORM_EPS = 1e-6
ROPE_THETA = 10000.0
MESH = pl.DeviceIdType.MESH


def rms_norm(values, gain_vec):
    vals_f32 = values.astype(jnp.float32)
    inv_rms = lax.rsqrt(jnp.mean(vals_f32 * vals_f32, axis=-1, keepdims=True) + NORM_EPS)
    return (vals_f32 * inv_rms * gain_vec.astype(jnp.float32)).astype(jnp.bfloat16)


def rope_tables(positions, rope_dim):
    inv_freq = ROPE_THETA ** (-2.0 * jnp.arange(rope_dim // 2, dtype=jnp.float32) / rope_dim)
    angles = positions.astype(jnp.float32)[:, None] * inv_freq[None, :]
    return jnp.cos(angles), jnp.sin(angles)


def apply_rope(values, rope_cos, rope_sin):
    half_dim = values.shape[-1] // 2
    first_half = values[..., :half_dim]
    second_half = values[..., half_dim:]
    return jnp.concatenate([first_half * rope_cos - second_half * rope_sin, second_half * rope_cos + first_half * rope_sin], axis=-1)


def attention_block(hidden, ckv_cache, kr_cache, seq_lens, attn_gain, kv_gain, w_q, w_dkv, w_uk, w_uv, w_o):
    batch_rows = hidden.shape[0]
    num_heads, nope_dim, value_a8 = w_uk.shape
    rope_dim = kr_cache.shape[-1]
    cache_len = ckv_cache.shape[1]
    score_scale = (nope_dim + rope_dim) ** -0.5
    normed_x = rms_norm(hidden, attn_gain)
    q_all = jnp.dot(normed_x, w_q, preferred_element_type=jnp.float32).astype(jnp.bfloat16).reshape(batch_rows, num_heads, nope_dim + rope_dim)
    latent_kv = jnp.dot(normed_x, w_dkv, preferred_element_type=jnp.float32)
    ckv_new = rms_norm(latent_kv[:, :value_a8], kv_gain)
    rope_cos, rope_sin = rope_tables(seq_lens, rope_dim)
    kr_new = apply_rope(latent_kv[:, value_a8:], rope_cos, rope_sin).astype(jnp.bfloat16)
    q_rot = apply_rope(q_all[:, :, nope_dim:].astype(jnp.float32), rope_cos[:, None, :], rope_sin[:, None, :]).astype(jnp.bfloat16)
    q_lat = jnp.einsum('bhn,hnc->bhc', q_all[:, :, :nope_dim], w_uk, preferred_element_type=jnp.float32).astype(jnp.bfloat16)
    scores = (jnp.einsum('bhc,blc->bhl', q_lat, ckv_cache, preferred_element_type=jnp.float32) + jnp.einsum('bhr,blr->bhl', q_rot, kr_cache, preferred_element_type=jnp.float32)) * score_scale
    valid_mask = jnp.arange(cache_len)[None, None, :] < seq_lens[:, None, None]
    scores = jnp.where(valid_mask, scores, -jnp.inf)
    new_score = (jnp.einsum('bhc,bc->bh', q_lat, ckv_new, preferred_element_type=jnp.float32) + jnp.einsum('bhr,br->bh', q_rot, kr_new, preferred_element_type=jnp.float32)) * score_scale
    top_score = jnp.maximum(jnp.max(scores, axis=-1), new_score)
    exp_cache = jnp.exp(scores - top_score[:, :, None])
    exp_new = jnp.exp(new_score - top_score)
    denominator = jnp.sum(exp_cache, axis=-1) + exp_new
    prob_cache = (exp_cache / denominator[:, :, None]).astype(jnp.bfloat16)
    prob_new = (exp_new / denominator).astype(jnp.bfloat16)
    o_lat = (jnp.einsum('bhl,blc->bhc', prob_cache, ckv_cache, preferred_element_type=jnp.float32) + jnp.einsum('bh,bc->bhc', prob_new, ckv_new, preferred_element_type=jnp.float32)).astype(jnp.bfloat16)
    head_out = jnp.einsum('bhc,hcv->bhv', o_lat, w_uv, preferred_element_type=jnp.float32).astype(jnp.bfloat16).reshape(batch_rows, -1)
    resid_out = (hidden.astype(jnp.float32) + jnp.dot(head_out, w_o, preferred_element_type=jnp.float32)).astype(jnp.bfloat16)
    return resid_out, ckv_new, kr_new


def moe_kernel(axis, topo, u_ref, g_ref, a_ref, sg_hbm, su_hbm, sd_hbm, eg_hbm, eu_hbm, ed_hbm, out_ref,
               u_all, g_all, x_buf, oht_buf, g_loc, acc_buf, mid_buf, y_buf, s_acc, part, px, ring_in,
               sgu_buf, sd_buf, gu_buf, dn_buf,
               sgu_sem, sd_sem, gu_sem, dn_sem,
               agu_send, agu_recv, agg_send, agg_recv, pru_send, pru_recv, prg_send, prg_recv,
               px_send, px_recv, rs_send, rs_recv):
    num_devs, half_steps = topo
    ring_len = num_devs // 2
    me = lax.axis_index(axis)
    ring_pos = me // 2
    core = me % 2
    up_dev = ((ring_pos + 1) % ring_len) * 2 + core
    down_dev = ((ring_pos + ring_len - 1) % ring_len) * 2 + core
    pair_dev = ring_pos * 2 + (1 - core)
    ring_dev = (up_dev, down_dev)
    rows, width = u_ref.shape
    half_rows = rows // 2
    local_experts, _, ff_dim = eg_hbm.shape
    shared_chunk = sd_buf.shape[1]
    num_shared = sd_hbm.shape[0] // shared_chunk
    shared_slots = sd_buf.shape[0]
    k_chunk = gu_buf.shape[1]
    num_k = width // k_chunk
    num_gu = local_experts * num_k
    gu_slots = gu_buf.shape[0]
    col_chunk = dn_buf.shape[2]
    num_cols = width // col_chunk
    num_dn = num_cols * local_experts
    dn_slots = dn_buf.shape[0]
    slots = x_buf.shape[1] // local_experts
    num_pieces = 2 * half_steps - 1

    def shared_copies(i):
        slot = lax.rem(i, shared_slots)
        off = pl.multiple_of(i * shared_chunk, shared_chunk)
        return (
            pltpu.make_async_copy(sg_hbm.at[:, pl.ds(off, shared_chunk)], sgu_buf.at[slot, :, pl.ds(0, shared_chunk)], sgu_sem.at[slot, 0]),
            pltpu.make_async_copy(su_hbm.at[:, pl.ds(off, shared_chunk)], sgu_buf.at[slot, :, pl.ds(shared_chunk, shared_chunk)], sgu_sem.at[slot, 1]),
            pltpu.make_async_copy(sd_hbm.at[pl.ds(off, shared_chunk), :], sd_buf.at[slot], sd_sem.at[slot]),
        )

    def gu_copies(j):
        slot = lax.rem(j, gu_slots)
        e = lax.div(j, num_k)
        off = pl.multiple_of(lax.rem(j, num_k) * k_chunk, k_chunk)
        return (
            pltpu.make_async_copy(eg_hbm.at[e, pl.ds(off, k_chunk), :], gu_buf.at[slot, :, pl.ds(0, ff_dim)], gu_sem.at[slot, 0]),
            pltpu.make_async_copy(eu_hbm.at[e, pl.ds(off, k_chunk), :], gu_buf.at[slot, :, pl.ds(ff_dim, ff_dim)], gu_sem.at[slot, 1]),
        )

    def dn_copy(q):
        slot = lax.rem(q, dn_slots)
        e = lax.rem(q, local_experts)
        off = pl.multiple_of(lax.div(q, local_experts) * col_chunk, col_chunk)
        return pltpu.make_async_copy(ed_hbm.at[e, :, pl.ds(off, col_chunk)], dn_buf.at[slot], dn_sem.at[slot])

    def start_all(copies):
        for cp in copies:
            cp.start()

    def wait_all(copies):
        for cp in copies:
            cp.wait()

    for i in range(min(shared_slots, num_shared)):
        start_all(shared_copies(i))

    barrier = pltpu.get_barrier_semaphore()
    for dev in (up_dev, down_dev, pair_dev):
        pl.semaphore_signal(barrier, inc=1, device_id={axis: dev}, device_id_type=MESH)
    pl.semaphore_wait(barrier, 3)

    def piece_rows(direction, p):
        half = lax.rem(p, 2)
        half = half if direction == 0 else 1 - half
        return pl.ds(pl.multiple_of(half * half_rows, half_rows), half_rows)

    def held_slot(direction, step):
        return lax.rem(ring_len - step, ring_len) if direction == 0 else step

    def gather_copies(direction, p, own):
        step = lax.div(p, 2)
        rws = piece_rows(direction, p)
        dst = held_slot(direction, step + 1)
        u_src = u_ref.at[rws] if own else u_all.at[0, held_slot(direction, step), rws]
        g_src = g_ref.at[rws] if own else g_all.at[0, held_slot(direction, step), rws]
        return (
            pltpu.make_async_remote_copy(src_ref=u_src, dst_ref=u_all.at[0, dst, rws], send_sem=agu_send.at[direction, p], recv_sem=agu_recv.at[direction, p], device_id={axis: ring_dev[direction]}, device_id_type=MESH),
            pltpu.make_async_remote_copy(src_ref=g_src, dst_ref=g_all.at[0, dst, rws], send_sem=agg_send.at[direction, p], recv_sem=agg_recv.at[direction, p], device_id={axis: ring_dev[direction]}, device_id_type=MESH),
        )

    def pair_copies(direction, p):
        rws = piece_rows(direction, p)
        slot = held_slot(direction, lax.div(p, 2) + 1)
        return (
            pltpu.make_async_remote_copy(src_ref=u_all.at[0, slot, rws], dst_ref=u_all.at[1, slot, rws], send_sem=pru_send.at[direction, p], recv_sem=pru_recv.at[direction, p], device_id={axis: pair_dev}, device_id_type=MESH),
            pltpu.make_async_remote_copy(src_ref=g_all.at[0, slot, rws], dst_ref=g_all.at[1, slot, rws], send_sem=prg_send.at[direction, p], recv_sem=prg_recv.at[direction, p], device_id={axis: pair_dev}, device_id_type=MESH),
        )

    pair_own = (
        pltpu.make_async_remote_copy(src_ref=u_ref, dst_ref=u_all.at[1, 0], send_sem=pru_send.at[0, num_pieces], recv_sem=pru_recv.at[0, num_pieces], device_id={axis: pair_dev}, device_id_type=MESH),
        pltpu.make_async_remote_copy(src_ref=g_ref, dst_ref=g_all.at[1, 0], send_sem=prg_send.at[0, num_pieces], recv_sem=prg_recv.at[0, num_pieces], device_id={axis: pair_dev}, device_id_type=MESH),
    )

    for p in range(2):
        for direction in range(2):
            start_all(gather_copies(direction, p, True))
    start_all(pair_own)
    u_all[0, 0] = u_ref[...]
    g_all[0, 0] = g_ref[...]

    def gather_event(p):
        for direction in range(2):
            for cp in gather_copies(direction, p, False):
                cp.wait_recv()

        @pl.when(p + 2 < num_pieces)
        def _():
            for direction in range(2):
                start_all(gather_copies(direction, p + 2, False))

        for direction in range(2):
            start_all(pair_copies(direction, p))

    s_acc[...] = jnp.zeros_like(s_acc)
    u_own = u_ref[...]

    def shared_step(i, carry):
        slot = lax.rem(i, shared_slots)
        wait_all(shared_copies(i))
        gu = jnp.dot(u_own, sgu_buf[slot], preferred_element_type=jnp.float32)
        act = (jax.nn.silu(gu[:, :shared_chunk]) * gu[:, shared_chunk:]).astype(jnp.bfloat16)
        s_acc[...] += jnp.dot(act, sd_buf[slot], preferred_element_type=jnp.float32)

        @pl.when(i + shared_slots < num_shared)
        def _():
            start_all(shared_copies(i + shared_slots))

        first_gu = num_shared - gu_slots

        @pl.when(i >= first_gu)
        def _():
            start_all(gu_copies(i - first_gu))

        turn = i - 2

        @pl.when((turn >= 0) & (lax.rem(turn + 3, 3) != 2))
        def _():
            gather_event(2 * lax.div(turn, 3) + lax.rem(turn, 3))

        return carry

    lax.fori_loop(0, num_shared, shared_step, 0)
    done_events = len([t for t in range(num_shared - 2) if t % 3 != 2])
    for p in range(done_events, num_pieces):
        gather_event(jnp.int32(p))
    for direction in range(2):
        for p in range(num_pieces):
            for cp in pair_copies(direction, p):
                cp.wait_recv()
    for cp in pair_own:
        cp.wait_recv()

    total_rows = num_devs * rows
    g_full = g_all[...].reshape(total_rows, g_all.shape[3])
    lanes = g_full.shape[1]
    g_mine = pltpu.roll(g_full, lax.rem(lanes - me * local_experts, lanes), 1)
    g_loc[...] = jnp.maximum(g_mine, 0.0)
    hit = g_mine >= 0.0
    row_i = lax.broadcasted_iota(jnp.int32, (total_rows, total_rows), 0)
    col_i = lax.broadcasted_iota(jnp.int32, (total_rows, total_rows), 1)
    before = jnp.where(col_i < row_i, 1.0, 0.0).astype(jnp.bfloat16)
    rank = jnp.dot(before, jnp.where(hit, 1.0, 0.0).astype(jnp.bfloat16), preferred_element_type=jnp.float32)
    place = jnp.where(hit, rank, -1.0)
    slot_i = lax.broadcasted_iota(jnp.int32, (total_rows, slots), 1).astype(jnp.float32)
    u_rows = u_all[...].reshape(total_rows, width)
    for e in range(local_experts):
        one_hot = jnp.where(slot_i == place[:, e:e + 1], 1.0, 0.0)
        oht_buf[e] = one_hot.astype(jnp.bfloat16)
        pick = one_hot.T.astype(jnp.bfloat16)
        for k in range(num_k):
            x_buf[k, e * slots:(e + 1) * slots] = jnp.dot(pick, u_rows[:, k * k_chunk:(k + 1) * k_chunk], preferred_element_type=jnp.float32).astype(jnp.bfloat16)

    def expert_step(e, carry):
        for k in range(num_k):
            j = e * num_k + k
            slot = lax.rem(j, gu_slots)
            wait_all(gu_copies(j))
            prod = jnp.dot(x_buf[k, pl.ds(pl.multiple_of(e * slots, slots), slots)], gu_buf[slot], preferred_element_type=jnp.float32)
            if k == 0:
                acc_buf[...] = prod
            else:
                acc_buf[...] += prod

            @pl.when(j + gu_slots < num_gu)
            def _():
                start_all(gu_copies(j + gu_slots))

            @pl.when((j + gu_slots >= num_gu) & (j + gu_slots - num_gu < dn_slots))
            def _():
                dn_copy(j + gu_slots - num_gu).start()

        mid_buf[e] = (jax.nn.silu(acc_buf[:, :ff_dim]) * acc_buf[:, ff_dim:]).astype(jnp.bfloat16)
        return carry

    lax.fori_loop(0, local_experts, expert_step, 0)
    for q in range(min(gu_slots, dn_slots), min(dn_slots, num_dn)):
        dn_copy(q).start()

    half_cols = col_chunk // 2

    def pair_sum_copy(c):
        return pltpu.make_async_remote_copy(src_ref=part.at[c, 1], dst_ref=px.at[c], send_sem=px_send.at[c], recv_sem=px_recv.at[c], device_id={axis: pair_dev}, device_id_type=MESH)

    def sum_slot(direction, step):
        return half_steps - step if direction == 0 else (half_steps + step) % ring_len

    def ring_copy(c, direction, step):
        slot = sum_slot(direction, step)
        if step == 0:
            cols = pl.ds(direction * half_cols, half_cols)
            src, dst = part.at[c, 0, slot, :, cols], ring_in.at[direction, c, step, :, cols]
        else:
            src, dst = part.at[c, 0, slot], ring_in.at[direction, c, step]
        return pltpu.make_async_remote_copy(src_ref=src, dst_ref=dst, send_sem=rs_send.at[direction, c, step], recv_sem=rs_recv.at[direction, c, step], device_id={axis: ring_dev[direction]}, device_id_type=MESH)

    def column_sums(c):
        def down_step(e, carry):
            q = c * local_experts + e
            slot = lax.rem(q, dn_slots)
            dn_copy(q).wait()
            y_buf[e] = jnp.dot(mid_buf[e], dn_buf[slot], preferred_element_type=jnp.float32).astype(jnp.bfloat16)

            @pl.when(q + dn_slots < num_dn)
            def _():
                dn_copy(q + dn_slots).start()

            return carry

        lax.fori_loop(0, local_experts, down_step, 0)
        total = None
        for e in range(local_experts):
            spread = jnp.dot(oht_buf[e], y_buf[e], preferred_element_type=jnp.float32) * g_loc[:, e:e + 1]
            total = spread if total is None else total + spread
        part[c] = total.reshape(2, ring_len, rows, col_chunk)
        pair_sum_copy(c).start()

    def ring_step(c, step):
        if step == 0:
            pair_sum_copy(c).wait_recv()
            part[c, 0, half_steps] += px[c, half_steps]
            for direction in range(2):
                ring_copy(c, direction, 0).start()
            return
        for direction in range(2):
            slot = sum_slot(direction, step)
            ring_copy(c, direction, step - 1).wait_recv()
            if step == 1:
                cols = slice(direction * half_cols, (direction + 1) * half_cols)
                part[c, 0, slot] += px[c, slot]
                part[c, 0, slot, :, cols] += ring_in[direction, c, 0, :, cols]
            elif step < half_steps:
                part[c, 0, slot] += px[c, slot] + ring_in[direction, c, step - 1]
            if step < half_steps:
                ring_copy(c, direction, step).start()
        if step == half_steps:
            cols = slice(c * col_chunk, (c + 1) * col_chunk)
            routed = part[c, 0, 0] + px[c, 0] + ring_in[0, c, step - 1] + ring_in[1, c, step - 1]
            out_ref[:, cols] = (a_ref[:, cols].astype(jnp.float32) + s_acc[:, cols] + routed).astype(jnp.bfloat16)

    for turn in range(num_cols + half_steps + 1):
        if turn < num_cols:
            column_sums(turn)
        for step in range(half_steps + 1):
            c = turn - 1 - step
            if 0 <= c < num_cols:
                ring_step(c, step)

    for direction in range(2):
        for p in range(num_pieces):
            for cp in gather_copies(direction, p, p < 2) + pair_copies(direction, p):
                cp.wait_send()
        for c in range(num_cols):
            for step in range(half_steps):
                ring_copy(c, direction, step).wait_send()
    for cp in pair_own:
        cp.wait_send()
    for c in range(num_cols):
        pair_sum_copy(c).wait_send()


def moe_call(axis, num_devs, moe_in, gate_rows, resid_out, shared_gate, shared_up, shared_down, expert_gate, expert_up, expert_down, slots):
    rows, width = moe_in.shape
    local_experts, _, ff_dim = expert_gate.shape
    shared_dim = shared_down.shape[0]
    ring_len = num_devs // 2
    half_steps = ring_len // 2
    shared_chunk = 256
    shared_slots = 3
    k_chunk = min(512, width // 2)
    num_k = width // k_chunk
    gu_slots = min(6, shared_dim // shared_chunk, local_experts * num_k)
    num_cols = 4
    col_chunk = width // num_cols
    dn_slots = 8
    num_pieces = 2 * half_steps - 1
    lanes = gate_rows.shape[1]
    f32, bf16 = jnp.float32, jnp.bfloat16
    vmem = pl.BlockSpec(memory_space=pltpu.VMEM)
    anym = pl.BlockSpec(memory_space=pl.ANY)
    dma = pltpu.SemaphoreType.DMA
    return pl.pallas_call(
        functools.partial(moe_kernel, axis, (num_devs, half_steps)),
        name='moe_ring',
        out_shape=jax.ShapeDtypeStruct((rows, width), bf16),
        in_specs=[vmem] * 3 + [anym] * 6,
        out_specs=vmem,
        scratch_shapes=[
            pltpu.VMEM((2, ring_len, rows, width), bf16),
            pltpu.VMEM((2, ring_len, rows, lanes), f32),
            pltpu.VMEM((num_k, local_experts * slots, k_chunk), bf16),
            pltpu.VMEM((local_experts, num_devs * rows, slots), bf16),
            pltpu.VMEM((num_devs * rows, lanes), f32),
            pltpu.VMEM((slots, 2 * ff_dim), f32),
            pltpu.VMEM((local_experts, slots, ff_dim), bf16),
            pltpu.VMEM((local_experts, slots, col_chunk), bf16),
            pltpu.VMEM((rows, width), f32),
            pltpu.VMEM((num_cols, 2, ring_len, rows, col_chunk), f32),
            pltpu.VMEM((num_cols, ring_len, rows, col_chunk), f32),
            pltpu.VMEM((2, num_cols, half_steps, rows, col_chunk), f32),
            pltpu.VMEM((shared_slots, width, 2 * shared_chunk), bf16),
            pltpu.VMEM((shared_slots, shared_chunk, width), bf16),
            pltpu.VMEM((gu_slots, k_chunk, 2 * ff_dim), bf16),
            pltpu.VMEM((dn_slots, ff_dim, col_chunk), bf16),
            dma((shared_slots, 2)), dma((shared_slots,)), dma((gu_slots, 2)), dma((dn_slots,)),
            dma((2, num_pieces)), dma((2, num_pieces)), dma((2, num_pieces)), dma((2, num_pieces)),
            dma((2, num_pieces + 1)), dma((2, num_pieces + 1)), dma((2, num_pieces + 1)), dma((2, num_pieces + 1)),
            dma((num_cols,)), dma((num_cols,)), dma((2, num_cols, half_steps)), dma((2, num_cols, half_steps)),
        ],
        compiler_params=pltpu.CompilerParams(collective_id=0, has_side_effects=True, vmem_limit_bytes=67043328),
    )(moe_in, gate_rows, resid_out, shared_gate, shared_up, shared_down, expert_gate, expert_up, expert_down)


def gate_table(moe_in, expert_ids, w_router, lanes):
    num_experts = w_router.shape[1]
    router_prob = jax.nn.softmax(jnp.dot(moe_in, w_router, preferred_element_type=jnp.float32), axis=-1)
    picked = jnp.any(expert_ids[:, :, None] == jnp.arange(num_experts)[None, None, :], axis=1)
    return jnp.pad(jnp.where(picked, router_prob, -1.0), ((0, 0), (0, lanes - num_experts)), constant_values=-1.0)


def solution(mesh):
    row_spec = P(('rep', 'dp'))
    full_spec = P()
    expert_spec = P('dp')
    num_devs = mesh.shape['dp']

    def device_step(hidden, ckv_cache, kr_cache, seq_lens, expert_ids, attn_gain, kv_gain, moe_gain, w_q, w_dkv, w_uk, w_uv, w_o, w_router, shared_gate, shared_up, shared_down, expert_gate, expert_up, expert_down):
        num_experts = w_router.shape[1]
        capacity = max(2, 2 * hidden.shape[0] * expert_ids.shape[1] // num_experts)
        slots = -(-capacity * num_devs // 128) * 128
        lanes = -(-num_experts // 128) * 128
        resid_out, ckv_new, kr_new = attention_block(hidden, ckv_cache, kr_cache, seq_lens, attn_gain, kv_gain, w_q, w_dkv, w_uk, w_uv, w_o)
        moe_in = rms_norm(resid_out, moe_gain)
        gate_rows = gate_table(moe_in, expert_ids, w_router, lanes)
        layer_out = moe_call('dp', num_devs, moe_in, gate_rows, resid_out, shared_gate, shared_up, shared_down, expert_gate, expert_up, expert_down, slots)
        return layer_out, ckv_new, kr_new

    in_specs = (row_spec,) * 5 + (full_spec,) * 12 + (expert_spec,) * 3
    return jax.shard_map(device_step, mesh=mesh, in_specs=in_specs, out_specs=(row_spec, row_spec, row_spec), check_vma=False)
```

```python
import functools

import jax
import jax.numpy as jnp
from jax import lax
from jax.experimental import pallas as pl
from jax.experimental.pallas import tpu as pltpu
from jax.sharding import PartitionSpec as P

NORM_EPS = 1e-6
ROPE_THETA = 10000.0
MESH = pl.DeviceIdType.MESH


def rms_norm(values, gain_vec):
    vals_f32 = values.astype(jnp.float32)
    inv_rms = lax.rsqrt(jnp.mean(vals_f32 * vals_f32, axis=-1, keepdims=True) + NORM_EPS)
    return (vals_f32 * inv_rms * gain_vec.astype(jnp.float32)).astype(jnp.bfloat16)


def rope_tables(positions, rope_dim):
    inv_freq = ROPE_THETA ** (-2.0 * jnp.arange(rope_dim // 2, dtype=jnp.float32) / rope_dim)
    angles = positions.astype(jnp.float32)[:, None] * inv_freq[None, :]
    return jnp.cos(angles), jnp.sin(angles)


def apply_rope(values, rope_cos, rope_sin):
    half_dim = values.shape[-1] // 2
    first_half = values[..., :half_dim]
    second_half = values[..., half_dim:]
    return jnp.concatenate([first_half * rope_cos - second_half * rope_sin, second_half * rope_cos + first_half * rope_sin], axis=-1)


def attention_block(hidden, ckv_cache, kr_cache, seq_lens, attn_gain, kv_gain, w_q, w_dkv, w_uk, w_uv, w_o):
    batch_rows = hidden.shape[0]
    num_heads, nope_dim, value_a8 = w_uk.shape
    rope_dim = kr_cache.shape[-1]
    cache_len = ckv_cache.shape[1]
    score_scale = (nope_dim + rope_dim) ** -0.5
    normed_x = rms_norm(hidden, attn_gain)
    q_all = jnp.dot(normed_x, w_q, preferred_element_type=jnp.float32).astype(jnp.bfloat16).reshape(batch_rows, num_heads, nope_dim + rope_dim)
    latent_kv = jnp.dot(normed_x, w_dkv, preferred_element_type=jnp.float32)
    ckv_new = rms_norm(latent_kv[:, :value_a8], kv_gain)
    rope_cos, rope_sin = rope_tables(seq_lens, rope_dim)
    kr_new = apply_rope(latent_kv[:, value_a8:], rope_cos, rope_sin).astype(jnp.bfloat16)
    q_rot = apply_rope(q_all[:, :, nope_dim:].astype(jnp.float32), rope_cos[:, None, :], rope_sin[:, None, :]).astype(jnp.bfloat16)
    q_lat = jnp.einsum('bhn,hnc->bhc', q_all[:, :, :nope_dim], w_uk, preferred_element_type=jnp.float32).astype(jnp.bfloat16)
    scores = (jnp.einsum('bhc,blc->bhl', q_lat, ckv_cache, preferred_element_type=jnp.float32) + jnp.einsum('bhr,blr->bhl', q_rot, kr_cache, preferred_element_type=jnp.float32)) * score_scale
    valid_mask = jnp.arange(cache_len)[None, None, :] < seq_lens[:, None, None]
    scores = jnp.where(valid_mask, scores, -jnp.inf)
    new_score = (jnp.einsum('bhc,bc->bh', q_lat, ckv_new, preferred_element_type=jnp.float32) + jnp.einsum('bhr,br->bh', q_rot, kr_new, preferred_element_type=jnp.float32)) * score_scale
    top_score = jnp.maximum(jnp.max(scores, axis=-1), new_score)
    exp_cache = jnp.exp(scores - top_score[:, :, None])
    exp_new = jnp.exp(new_score - top_score)
    denominator = jnp.sum(exp_cache, axis=-1) + exp_new
    prob_cache = (exp_cache / denominator[:, :, None]).astype(jnp.bfloat16)
    prob_new = (exp_new / denominator).astype(jnp.bfloat16)
    o_lat = (jnp.einsum('bhl,blc->bhc', prob_cache, ckv_cache, preferred_element_type=jnp.float32) + jnp.einsum('bh,bc->bhc', prob_new, ckv_new, preferred_element_type=jnp.float32)).astype(jnp.bfloat16)
    head_out = jnp.einsum('bhc,hcv->bhv', o_lat, w_uv, preferred_element_type=jnp.float32).astype(jnp.bfloat16).reshape(batch_rows, -1)
    resid_out = (hidden.astype(jnp.float32) + jnp.dot(head_out, w_o, preferred_element_type=jnp.float32)).astype(jnp.bfloat16)
    return resid_out, ckv_new, kr_new


def moe_kernel(axis, topo, u_ref, g_ref, a_ref, sg_hbm, su_hbm, sd_hbm, eg_hbm, eu_hbm, ed_hbm, out_ref,
               u_all, g_all, x_buf, oht_buf, g_loc, acc_buf, mid_buf, shared_mid, y_buf, s_acc, part, px, ring_in,
               gu_buf, dn_buf, gu_sem, dn_sem,
               agu_send, agu_recv, agg_send, agg_recv, pru_send, pru_recv, prg_send, prg_recv,
               px_send, px_recv, rs_send, rs_recv):
    num_devs, half_steps = topo
    ring_len = num_devs // 2
    me = lax.axis_index(axis)
    ring_pos = me // 2
    core = me % 2
    up_dev = ((ring_pos + 1) % ring_len) * 2 + core
    down_dev = ((ring_pos + ring_len - 1) % ring_len) * 2 + core
    pair_dev = ring_pos * 2 + (1 - core)
    ring_dev = (up_dev, down_dev)
    rows, width = u_ref.shape
    half_rows = rows // 2
    local_experts, _, ff_dim = eg_hbm.shape
    k_chunk = gu_buf.shape[1]
    num_k = width // k_chunk
    num_gu = local_experts * num_k
    gu_slots = gu_buf.shape[0]
    col_chunk = dn_buf.shape[2]
    num_cols = width // col_chunk
    num_dn = num_cols * local_experts
    dn_slots = dn_buf.shape[0]
    slots = x_buf.shape[1] // local_experts
    num_shared_gu = 2 * num_k
    num_shared_dn = 2 * num_cols
    num_pieces = 2 * half_steps - 1

    def gu_copies(j):
        slot = lax.rem(j, gu_slots)
        e = lax.div(j, num_k)
        off = pl.multiple_of(lax.rem(j, num_k) * k_chunk, k_chunk)
        return (
            pltpu.make_async_copy(eg_hbm.at[e, pl.ds(off, k_chunk), :], gu_buf.at[slot, :, pl.ds(0, ff_dim)], gu_sem.at[slot, 0]),
            pltpu.make_async_copy(eu_hbm.at[e, pl.ds(off, k_chunk), :], gu_buf.at[slot, :, pl.ds(ff_dim, ff_dim)], gu_sem.at[slot, 1]),
        )

    def shared_gu_copy(j):
        src = (sg_hbm, su_hbm)[j // num_k]
        slot = (num_gu + j) % gu_slots
        return pltpu.make_async_copy(src.at[pl.ds((j % num_k) * k_chunk, k_chunk), :], gu_buf.at[slot], gu_sem.at[slot, 0])

    def shared_dn_copy(q):
        slot = (num_dn + q) % dn_slots
        rws = pl.ds((q % 2) * ff_dim, ff_dim)
        return pltpu.make_async_copy(sd_hbm.at[rws, pl.ds((q // 2) * col_chunk, col_chunk)], dn_buf.at[slot], dn_sem.at[slot])

    def dn_copy(q):
        slot = lax.rem(q, dn_slots)
        e = lax.rem(q, local_experts)
        off = pl.multiple_of(lax.div(q, local_experts) * col_chunk, col_chunk)
        return pltpu.make_async_copy(ed_hbm.at[e, :, pl.ds(off, col_chunk)], dn_buf.at[slot], dn_sem.at[slot])

    def start_all(copies):
        for cp in copies:
            cp.start()

    def wait_all(copies):
        for cp in copies:
            cp.wait()

    for j in range(gu_slots):
        start_all(gu_copies(j))
    for q in range(dn_slots):
        dn_copy(q).start()

    barrier = pltpu.get_barrier_semaphore()
    for dev in (up_dev, down_dev, pair_dev):
        pl.semaphore_signal(barrier, inc=1, device_id={axis: dev}, device_id_type=MESH)
    pl.semaphore_wait(barrier, 3)

    def piece_rows(direction, p):
        half = p % 2 if direction == 0 else 1 - p % 2
        return pl.ds(half * half_rows, half_rows)

    def held_slot(direction, step):
        return (ring_len - step) % ring_len if direction == 0 else step

    def gather_copies(direction, p, own):
        step = p // 2
        rws = piece_rows(direction, p)
        dst = held_slot(direction, step + 1)
        u_src = u_ref.at[rws] if own else u_all.at[0, held_slot(direction, step), rws]
        g_src = g_ref.at[rws] if own else g_all.at[0, held_slot(direction, step), rws]
        return (
            pltpu.make_async_remote_copy(src_ref=u_src, dst_ref=u_all.at[0, dst, rws], send_sem=agu_send.at[direction, p], recv_sem=agu_recv.at[direction, p], device_id={axis: ring_dev[direction]}, device_id_type=MESH),
            pltpu.make_async_remote_copy(src_ref=g_src, dst_ref=g_all.at[0, dst, rws], send_sem=agg_send.at[direction, p], recv_sem=agg_recv.at[direction, p], device_id={axis: ring_dev[direction]}, device_id_type=MESH),
        )

    def pair_copies(direction, p):
        rws = piece_rows(direction, p)
        slot = held_slot(direction, p // 2 + 1)
        return (
            pltpu.make_async_remote_copy(src_ref=u_all.at[0, slot, rws], dst_ref=u_all.at[1, slot, rws], send_sem=pru_send.at[direction, p], recv_sem=pru_recv.at[direction, p], device_id={axis: pair_dev}, device_id_type=MESH),
            pltpu.make_async_remote_copy(src_ref=g_all.at[0, slot, rws], dst_ref=g_all.at[1, slot, rws], send_sem=prg_send.at[direction, p], recv_sem=prg_recv.at[direction, p], device_id={axis: pair_dev}, device_id_type=MESH),
        )

    pair_own = (
        pltpu.make_async_remote_copy(src_ref=u_ref, dst_ref=u_all.at[1, 0], send_sem=pru_send.at[0, num_pieces], recv_sem=pru_recv.at[0, num_pieces], device_id={axis: pair_dev}, device_id_type=MESH),
        pltpu.make_async_remote_copy(src_ref=g_ref, dst_ref=g_all.at[1, 0], send_sem=prg_send.at[0, num_pieces], recv_sem=prg_recv.at[0, num_pieces], device_id={axis: pair_dev}, device_id_type=MESH),
    )

    for p in range(2):
        for direction in range(2):
            start_all(gather_copies(direction, p, True))
    start_all(pair_own)
    u_all[0, 0] = u_ref[...]
    g_all[0, 0] = g_ref[...]

    def gather_event(p):
        for direction in range(2):
            for cp in gather_copies(direction, p, False):
                cp.wait_recv()

        if p + 2 < num_pieces:
            for direction in range(2):
                start_all(gather_copies(direction, p + 2, False))
        for direction in range(2):
            start_all(pair_copies(direction, p))

    for p in range(num_pieces):
        gather_event(p)
    for direction in range(2):
        for p in range(num_pieces):
            for cp in pair_copies(direction, p):
                cp.wait_recv()
    for cp in pair_own:
        cp.wait_recv()

    total_rows = num_devs * rows
    g_full = g_all[...].reshape(total_rows, g_all.shape[3])
    lanes = g_full.shape[1]
    g_mine = pltpu.roll(g_full, lax.rem(lanes - me * local_experts, lanes), 1)
    g_loc[...] = jnp.maximum(g_mine, 0.0)
    hit = g_mine >= 0.0
    row_i = lax.broadcasted_iota(jnp.int32, (total_rows, total_rows), 0)
    col_i = lax.broadcasted_iota(jnp.int32, (total_rows, total_rows), 1)
    before = jnp.where(col_i < row_i, 1.0, 0.0).astype(jnp.bfloat16)
    rank = jnp.dot(before, jnp.where(hit, 1.0, 0.0).astype(jnp.bfloat16), preferred_element_type=jnp.float32)
    place = jnp.where(hit, rank, -1.0)
    slot_i = lax.broadcasted_iota(jnp.int32, (total_rows, slots), 1).astype(jnp.float32)
    u_rows = u_all[...].reshape(total_rows, width)
    for e in range(local_experts):
        one_hot = jnp.where(slot_i == place[:, e:e + 1], 1.0, 0.0)
        oht_buf[e] = one_hot.astype(jnp.bfloat16)
        pick = one_hot.T.astype(jnp.bfloat16)
        for k in range(num_k):
            x_buf[k, e * slots:(e + 1) * slots] = jnp.dot(pick, u_rows[:, k * k_chunk:(k + 1) * k_chunk], preferred_element_type=jnp.float32).astype(jnp.bfloat16)

    def expert_step(e, carry):
        for k in range(num_k):
            j = e * num_k + k
            slot = lax.rem(j, gu_slots)
            wait_all(gu_copies(j))
            prod = jnp.dot(x_buf[k, pl.ds(pl.multiple_of(e * slots, slots), slots)], gu_buf[slot], preferred_element_type=jnp.float32)
            if k == 0:
                acc_buf[...] = prod
            else:
                acc_buf[...] += prod

            @pl.when(j + gu_slots < num_gu)
            def _():
                start_all(gu_copies(j + gu_slots))

        mid_buf[e] = (jax.nn.silu(acc_buf[:, :ff_dim]) * acc_buf[:, ff_dim:]).astype(jnp.bfloat16)
        return carry

    lax.fori_loop(0, local_experts, expert_step, 0)
    half_cols = col_chunk // 2

    def pair_sum_copy(c):
        return pltpu.make_async_remote_copy(src_ref=part.at[c, 1], dst_ref=px.at[c], send_sem=px_send.at[c], recv_sem=px_recv.at[c], device_id={axis: pair_dev}, device_id_type=MESH)

    def sum_slot(direction, step):
        return half_steps - step if direction == 0 else (half_steps + step) % ring_len

    def ring_copy(c, direction, step):
        slot = sum_slot(direction, step)
        if step == 0:
            cols = pl.ds(direction * half_cols, half_cols)
            src, dst = part.at[c, 0, slot, :, cols], ring_in.at[direction, c, step, :, cols]
        else:
            src, dst = part.at[c, 0, slot], ring_in.at[direction, c, step]
        return pltpu.make_async_remote_copy(src_ref=src, dst_ref=dst, send_sem=rs_send.at[direction, c, step], recv_sem=rs_recv.at[direction, c, step], device_id={axis: ring_dev[direction]}, device_id_type=MESH)

    def column_sums(c):
        for e in range(local_experts):
            q = c * local_experts + e
            dn_copy(q).wait()
            y_buf[e] = jnp.dot(mid_buf[e], dn_buf[q % dn_slots], preferred_element_type=jnp.float32).astype(jnp.bfloat16)
            ahead = q + dn_slots
            if ahead < num_dn:
                dn_copy(ahead).start()
            else:
                if ahead - num_dn < num_shared_gu:
                    shared_gu_copy(ahead - num_dn).start()
                if ahead - num_dn < num_shared_dn:
                    shared_dn_copy(ahead - num_dn).start()
        total = None
        for e in range(local_experts):
            spread = jnp.dot(oht_buf[e], y_buf[e], preferred_element_type=jnp.float32) * g_loc[:, e:e + 1]
            total = spread if total is None else total + spread
        part[c] = total.reshape(2, ring_len, rows, col_chunk)
        pair_sum_copy(c).start()

    def ring_step(c, step):
        if step == 0:
            pair_sum_copy(c).wait_recv()
            part[c, 0, half_steps] += px[c, half_steps]
            for direction in range(2):
                ring_copy(c, direction, 0).start()
            return
        for direction in range(2):
            slot = sum_slot(direction, step)
            ring_copy(c, direction, step - 1).wait_recv()
            if step == 1:
                cols = slice(direction * half_cols, (direction + 1) * half_cols)
                part[c, 0, slot] += px[c, slot]
                part[c, 0, slot, :, cols] += ring_in[direction, c, 0, :, cols]
            elif step < half_steps:
                part[c, 0, slot] += px[c, slot] + ring_in[direction, c, step - 1]
            if step < half_steps:
                ring_copy(c, direction, step).start()
        if step == half_steps:
            part[c, 0, 0] += px[c, 0] + ring_in[0, c, step - 1] + ring_in[1, c, step - 1]

    def shared_gu(j):
        shared_gu_copy(j).wait()
        k = j % num_k
        rws = pl.ds((j // num_k) * rows, rows)
        prod = jnp.dot(u_ref[:, k * k_chunk:(k + 1) * k_chunk], gu_buf[(num_gu + j) % gu_slots], preferred_element_type=jnp.float32)
        if k == 0:
            acc_buf[rws] = prod
        else:
            acc_buf[rws] += prod
        if j == num_shared_gu - 1:
            act = (jax.nn.silu(acc_buf[:rows]) * acc_buf[rows:2 * rows]).astype(jnp.bfloat16)
            for h in range(2):
                shared_mid[h] = act[:, h * ff_dim:(h + 1) * ff_dim]

    def shared_dn(q):
        shared_dn_copy(q).wait()
        cols = slice((q // 2) * col_chunk, (q // 2 + 1) * col_chunk)
        prod = jnp.dot(shared_mid[q % 2], dn_buf[(num_dn + q) % dn_slots], preferred_element_type=jnp.float32)
        if q % 2 == 0:
            s_acc[:, cols] = prod
        else:
            s_acc[:, cols] += prod

    fillers = [functools.partial(shared_gu, j) for j in range(num_shared_gu)] + [functools.partial(shared_dn, q) for q in range(num_shared_dn)]

    for turn in range(num_cols + half_steps + 1):
        if turn < num_cols:
            column_sums(turn)
        for step in range(half_steps + 1):
            c = turn - 1 - step
            if 0 <= c < num_cols:
                ring_step(c, step)
                if turn >= num_cols:
                    for filler in fillers[:2]:
                        filler()
                    fillers = fillers[2:]
    for filler in fillers:
        filler()
    for c in range(num_cols):
        cols = slice(c * col_chunk, (c + 1) * col_chunk)
        out_ref[:, cols] = (a_ref[:, cols].astype(jnp.float32) + s_acc[:, cols] + part[c, 0, 0]).astype(jnp.bfloat16)

    for direction in range(2):
        for p in range(num_pieces):
            for cp in gather_copies(direction, p, p < 2) + pair_copies(direction, p):
                cp.wait_send()
        for c in range(num_cols):
            for step in range(half_steps):
                ring_copy(c, direction, step).wait_send()
    for cp in pair_own:
        cp.wait_send()
    for c in range(num_cols):
        pair_sum_copy(c).wait_send()


def moe_call(axis, num_devs, moe_in, gate_rows, resid_out, shared_gate, shared_up, shared_down, expert_gate, expert_up, expert_down, slots):
    rows, width = moe_in.shape
    local_experts, _, ff_dim = expert_gate.shape
    assert shared_down.shape[0] == 2 * ff_dim
    ring_len = num_devs // 2
    half_steps = ring_len // 2
    k_chunk = min(512, width // 2)
    num_k = width // k_chunk
    gu_slots = min(10, local_experts * num_k)
    num_cols = 4
    col_chunk = width // num_cols
    dn_slots = 10
    num_pieces = 2 * half_steps - 1
    lanes = gate_rows.shape[1]
    f32, bf16 = jnp.float32, jnp.bfloat16
    vmem = pl.BlockSpec(memory_space=pltpu.VMEM)
    anym = pl.BlockSpec(memory_space=pl.ANY)
    dma = pltpu.SemaphoreType.DMA
    return pl.pallas_call(
        functools.partial(moe_kernel, axis, (num_devs, half_steps)),
        name='moe_ring',
        out_shape=jax.ShapeDtypeStruct((rows, width), bf16),
        in_specs=[vmem] * 3 + [anym] * 6,
        out_specs=vmem,
        scratch_shapes=[
            pltpu.VMEM((2, ring_len, rows, width), bf16),
            pltpu.VMEM((2, ring_len, rows, lanes), f32),
            pltpu.VMEM((num_k, local_experts * slots, k_chunk), bf16),
            pltpu.VMEM((local_experts, num_devs * rows, slots), bf16),
            pltpu.VMEM((num_devs * rows, lanes), f32),
            pltpu.VMEM((slots, 2 * ff_dim), f32),
            pltpu.VMEM((local_experts, slots, ff_dim), bf16),
            pltpu.VMEM((2, rows, ff_dim), bf16),
            pltpu.VMEM((local_experts, slots, col_chunk), bf16),
            pltpu.VMEM((rows, width), f32),
            pltpu.VMEM((num_cols, 2, ring_len, rows, col_chunk), f32),
            pltpu.VMEM((num_cols, ring_len, rows, col_chunk), f32),
            pltpu.VMEM((2, num_cols, half_steps, rows, col_chunk), f32),
            pltpu.VMEM((gu_slots, k_chunk, 2 * ff_dim), bf16),
            pltpu.VMEM((dn_slots, ff_dim, col_chunk), bf16),
            dma((gu_slots, 2)), dma((dn_slots,)),
            dma((2, num_pieces)), dma((2, num_pieces)), dma((2, num_pieces)), dma((2, num_pieces)),
            dma((2, num_pieces + 1)), dma((2, num_pieces + 1)), dma((2, num_pieces + 1)), dma((2, num_pieces + 1)),
            dma((num_cols,)), dma((num_cols,)), dma((2, num_cols, half_steps)), dma((2, num_cols, half_steps)),
        ],
        compiler_params=pltpu.CompilerParams(collective_id=0, has_side_effects=True, vmem_limit_bytes=67043328),
    )(moe_in, gate_rows, resid_out, shared_gate, shared_up, shared_down, expert_gate, expert_up, expert_down)


def gate_table(moe_in, expert_ids, w_router, lanes):
    num_experts = w_router.shape[1]
    router_prob = jax.nn.softmax(jnp.dot(moe_in, w_router, preferred_element_type=jnp.float32), axis=-1)
    picked = jnp.any(expert_ids[:, :, None] == jnp.arange(num_experts)[None, None, :], axis=1)
    return jnp.pad(jnp.where(picked, router_prob, -1.0), ((0, 0), (0, lanes - num_experts)), constant_values=-1.0)


def solution(mesh):
    row_spec = P(('rep', 'dp'))
    full_spec = P()
    expert_spec = P('dp')
    num_devs = mesh.shape['dp']

    def device_step(hidden, ckv_cache, kr_cache, seq_lens, expert_ids, attn_gain, kv_gain, moe_gain, w_q, w_dkv, w_uk, w_uv, w_o, w_router, shared_gate, shared_up, shared_down, expert_gate, expert_up, expert_down):
        num_experts = w_router.shape[1]
        capacity = max(2, 2 * hidden.shape[0] * expert_ids.shape[1] // num_experts)
        slots = -(-capacity * num_devs // 128) * 128
        lanes = -(-num_experts // 128) * 128
        resid_out, ckv_new, kr_new = attention_block(hidden, ckv_cache, kr_cache, seq_lens, attn_gain, kv_gain, w_q, w_dkv, w_uk, w_uv, w_o)
        moe_in = rms_norm(resid_out, moe_gain)
        gate_rows = gate_table(moe_in, expert_ids, w_router, lanes)
        layer_out = moe_call('dp', num_devs, moe_in, gate_rows, resid_out, shared_gate, shared_up, shared_down, expert_gate, expert_up, expert_down, slots)
        return layer_out, ckv_new, kr_new

    in_specs = (row_spec,) * 5 + (full_spec,) * 12 + (expert_spec,) * 3
    return jax.shard_map(device_step, mesh=mesh, in_specs=in_specs, out_specs=(row_spec, row_spec, row_spec), check_vma=False)
```

```python
import functools
import math

import jax
import jax.numpy as jnp
from jax import lax
from jax.experimental import pallas as pl
from jax.experimental.pallas import tpu as pltpu
from jax.sharding import PartitionSpec as P

NORM_EPS = 1e-6
ROPE_THETA = 10000.0
MESH = pl.DeviceIdType.MESH


def attn_kernel(dims, lens_smem, lens_ref, ids_ref, hid_ref, ag_ref, kg_ref, mg_ref, wq_hbm, wdkv_hbm, wuk_hbm, wuv_hbm, wo_hbm, wr_ref, ckv_hbm, kr_hbm,
                a_ref, u_ref, g_ref, ckvn_ref, krn_ref,
                wq, wdkv, wuk, wuv, wo, ckv, kr, q_lat, q_rot, o_lat, head_out, gate_t,
                wq_sem, wdkv_sem, wuk_sem, wuv_sem, wo_sem, ckv_sem, kr_sem):
    heads, nope_dim, rope_dim, latent, seq_block = dims
    bf16, f32 = jnp.bfloat16, jnp.float32
    rows, width = hid_ref.shape
    cache_len = ckv_hbm.shape[1]
    head_dim = nope_dim + rope_dim
    v_dim = wuv_hbm.shape[2]
    q_chunks = wq_sem.shape[0]
    q_cols = wq_hbm.shape[1] // q_chunks
    uk_chunks = wuk_sem.shape[0]
    uk_heads = heads // uk_chunks
    o_chunks = wo_sem.shape[0]
    o_rows = wo_hbm.shape[0] // o_chunks
    score_scale = head_dim ** -0.5
    tiles = latent // 128

    wq_cp = [pltpu.make_async_copy(wq_hbm.at[:, pl.ds(i * q_cols, q_cols)], wq.at[i], wq_sem.at[i]) for i in range(q_chunks)]
    wdkv_cp = pltpu.make_async_copy(wdkv_hbm, wdkv, wdkv_sem)
    wuk_cp = [pltpu.make_async_copy(wuk_hbm.at[pl.ds(i * uk_heads, uk_heads)], wuk.at[pl.ds(i * uk_heads, uk_heads)], wuk_sem.at[i]) for i in range(uk_chunks)]
    wuv_cp = pltpu.make_async_copy(wuv_hbm, wuv, wuv_sem)
    wo_cp = [pltpu.make_async_copy(wo_hbm.at[pl.ds(i * o_rows, o_rows)], wo.at[i], wo_sem.at[i]) for i in range(o_chunks)]
    seq_blocks = rows // seq_block
    ckv_cp = [pltpu.make_async_copy(ckv_hbm.at[pl.ds(i * seq_block, seq_block)], ckv.at[pl.ds(i * seq_block, seq_block)], ckv_sem.at[i]) for i in range(seq_blocks)]
    kr_cp = pltpu.make_async_copy(kr_hbm, kr, kr_sem)
    wdkv_cp.start()
    for i in range(q_chunks):
        wq_cp[i].start()
        if i * uk_chunks % q_chunks == 0:
            wuk_cp[i * uk_chunks // q_chunks].start()
    kr_cp.start()
    for cp in ckv_cp:
        cp.start()
    wuv_cp.start()
    for cp in wo_cp:
        cp.start()

    def norm(vals, gain):
        inv = lax.rsqrt(jnp.mean(vals * vals, axis=-1, keepdims=True) + NORM_EPS)
        return (vals * inv * gain.astype(f32)).astype(bf16)

    def dot_t(left, right):
        return lax.dot_general(left, right, (((1,), (1,)), ((), ())), preferred_element_type=f32)

    hid = hid_ref[...].astype(f32)
    x = norm(hid, ag_ref[...])

    lane = lax.broadcasted_iota(jnp.int32, (rows, 2 * rope_dim), 1)
    pair = (lane % (rope_dim // 2)).astype(f32)
    inv_freq = jnp.exp(pair * (-2.0 / rope_dim * math.log(ROPE_THETA)))
    angles = lens_ref[...].astype(f32) * inv_freq
    rope_cos, rope_sin = jnp.cos(angles), jnp.sin(angles)
    first = (lane % rope_dim) < rope_dim // 2

    def rope(vals):
        swapped = jnp.where(first, -pltpu.roll(vals, 2 * rope_dim - rope_dim // 2, 1), pltpu.roll(vals, rope_dim // 2, 1))
        return (vals * rope_cos + swapped * rope_sin).astype(bf16)

    wdkv_cp.wait()
    latent_kv = dot_t(x, wdkv[...])
    ckv_new = norm(latent_kv[:, :latent], kg_ref[...])
    ckvn_ref[...] = ckv_new
    k_part = latent_kv[:, latent:latent + rope_dim]
    kr_new = rope(jnp.concatenate([k_part, k_part], axis=1))
    krn_ref[...] = kr_new[:, :rope_dim]

    for i in range(q_chunks):
        wq_cp[i].wait()
        q_part = jnp.dot(x, wq[i], preferred_element_type=f32).astype(bf16).astype(f32)
        chunk_heads = q_cols // head_dim
        if (i * chunk_heads) % uk_heads == 0:
            wuk_cp[i * chunk_heads // uk_heads].wait()
        for m in range(chunk_heads // 2):
            head = i * chunk_heads + 2 * m
            base = 2 * m * head_dim
            both = jnp.where(lane < rope_dim, q_part[:, base + nope_dim:base + nope_dim + 2 * rope_dim], q_part[:, base + nope_dim + 2 * rope_dim:base + 2 * head_dim])
            turned = rope(both).astype(f32)
            q_rot[pl.ds(head, rows, stride=heads), :] = jnp.where(lane < rope_dim, turned, 0.0)
            q_rot[pl.ds(head + 1, rows, stride=heads), :] = jnp.where(lane < rope_dim, pltpu.roll(turned, rope_dim, 1), 0.0)
            for h in range(2):
                q_nope = q_part[:, base + h * head_dim:base + h * head_dim + nope_dim].astype(bf16)
                lat = jnp.dot(q_nope, wuk[head + h], preferred_element_type=f32).astype(bf16).astype(f32)
                for t in range(tiles):
                    q_lat[t, pl.ds(head + h, rows, stride=heads), :] = lat[:, t * 128:(t + 1) * 128]

    kr_cp.wait()
    key_lane = lax.broadcasted_iota(jnp.int32, (heads, cache_len), 1)
    new_lane = lax.broadcasted_iota(jnp.int32, (heads, rows), 1)
    for i in range(seq_blocks):
        ckv_cp[i].wait()

    def attend(i, carry):
        base = pl.multiple_of(i * seq_block * heads, seq_block * heads)
        ql = jnp.concatenate([q_lat[t, pl.ds(base, seq_block * heads), :] for t in range(tiles)], axis=1).astype(bf16)
        qr = q_rot[pl.ds(base, seq_block * heads), :].astype(bf16)
        new_all = (dot_t(ql, ckv_new) + dot_t(qr[:, :rope_dim], kr_new[:, :rope_dim])) * score_scale
        probs_new = []
        for s in range(seq_block):
            b = i * seq_block + s
            part = slice(s * heads, (s + 1) * heads)
            keys = ckv[b]
            score = (dot_t(ql[part], keys) + jnp.dot(qr[part, :rope_dim], kr[b], preferred_element_type=f32)) * score_scale
            score = jnp.where(key_lane < lens_smem[b], score, -jnp.inf)
            new = jnp.where(new_lane == b, new_all[part], -jnp.inf)
            top = jnp.maximum(jnp.max(score, axis=-1, keepdims=True), jnp.max(new, axis=-1, keepdims=True))
            e_cache, e_new = jnp.exp(score - top), jnp.exp(new - top)
            denom = jnp.sum(e_cache, axis=-1, keepdims=True) + jnp.sum(e_new, axis=-1, keepdims=True)
            p_cache, p_new = (e_cache / denom).astype(bf16), (e_new / denom).astype(bf16)
            out = jnp.dot(p_cache, keys, preferred_element_type=f32) + jnp.dot(p_new, ckv_new, preferred_element_type=f32)
            out = out.astype(bf16).astype(f32)
            for t in range(tiles):
                o_lat[t, pl.ds(pl.multiple_of(base + s * heads, heads), heads), :] = out[:, t * 128:(t + 1) * 128]
        return carry

    lax.fori_loop(0, seq_blocks, attend, 0)

    wuv_cp.wait()
    for h in range(heads):
        lat = jnp.concatenate([o_lat[t, pl.ds(h, rows, stride=heads), :] for t in range(tiles)], axis=1).astype(bf16)
        head_out[:, h * v_dim:(h + 1) * v_dim] = jnp.dot(lat, wuv[h], preferred_element_type=f32).astype(bf16)

    total = hid
    for i in range(o_chunks):
        wo_cp[i].wait()
        total = total + jnp.dot(head_out[:, i * o_rows:(i + 1) * o_rows], wo[i], preferred_element_type=f32)
    resid = total.astype(bf16)
    a_ref[...] = resid
    moe_in = norm(resid.astype(f32), mg_ref[...])
    u_ref[...] = moe_in

    logits = dot_t(wr_ref[...], moe_in)
    top = jnp.max(logits, axis=0, keepdims=True)
    e_log = jnp.exp(logits - top)
    probs = e_log / jnp.sum(e_log, axis=0, keepdims=True)
    expert = lax.broadcasted_iota(jnp.int32, logits.shape, 0)
    picked = expert == ids_ref[0:1, :]
    for k in range(1, ids_ref.shape[0]):
        picked = picked | (expert == ids_ref[k:k + 1, :])
    gate_t[...] = jnp.full(gate_t.shape, -1.0, f32)
    gate_t[:logits.shape[0], :rows] = jnp.where(picked, probs, -1.0)
    g_ref[...] = gate_t[...].T[:rows]


def attn_call(hidden, ckv_cache, kr_cache, seq_lens, expert_ids, attn_gain, kv_gain, moe_gain, w_q, w_dkv, w_uk, w_uv, w_o, w_router):
    rows, width = hidden.shape
    heads, nope_dim, latent = w_uk.shape
    v_dim = w_uv.shape[2]
    rope_dim = kr_cache.shape[2]
    cache_len = ckv_cache.shape[1]
    seq_block, q_chunks, uk_chunks, o_chunks = 8, 4, 2, 4
    bf16, f32 = jnp.bfloat16, jnp.float32
    vmem = pl.BlockSpec(memory_space=pltpu.VMEM)
    anym = pl.BlockSpec(memory_space=pl.ANY)
    smem = pl.BlockSpec(memory_space=pltpu.SMEM)
    dma = pltpu.SemaphoreType.DMA
    shape = jax.ShapeDtypeStruct
    return pl.pallas_call(
        functools.partial(attn_kernel, (heads, nope_dim, rope_dim, latent, seq_block)),
        name='attention',
        out_shape=(shape((rows, width), bf16), shape((rows, width), bf16), shape((rows, 128), f32), shape((rows, latent), bf16), shape((rows, rope_dim), bf16)),
        in_specs=[smem] + [vmem] * 6 + [anym] * 5 + [vmem] + [anym] * 2,
        out_specs=(vmem,) * 5,
        scratch_shapes=[
            pltpu.VMEM((q_chunks, width, w_q.shape[1] // q_chunks), bf16),
            pltpu.VMEM((w_dkv.shape[1], width), bf16),
            pltpu.VMEM(w_uk.shape, bf16),
            pltpu.VMEM(w_uv.shape, bf16),
            pltpu.VMEM((o_chunks, w_o.shape[0] // o_chunks, width), bf16),
            pltpu.VMEM((rows, cache_len, latent), bf16),
            pltpu.VMEM((rows, rope_dim, cache_len), bf16),
            pltpu.VMEM((latent // 128, rows * heads, 128), f32),
            pltpu.VMEM((rows * heads, 2 * rope_dim), f32),
            pltpu.VMEM((latent // 128, rows * heads, 128), f32),
            pltpu.VMEM((rows, heads * v_dim), bf16),
            pltpu.VMEM((128, 128), f32),
            dma((q_chunks,)), dma, dma((uk_chunks,)), dma, dma((o_chunks,)), dma((rows // seq_block,)), dma,
        ],
        compiler_params=pltpu.CompilerParams(vmem_limit_bytes=60000000),
    )(seq_lens, seq_lens.reshape(rows, 1), expert_ids.T, hidden, attn_gain.reshape(1, -1), kv_gain.reshape(1, -1), moe_gain.reshape(1, -1),
      w_q, w_dkv.T, w_uk, w_uv, w_o, w_router.T, ckv_cache, kr_cache.transpose(0, 2, 1))


def moe_kernel(axis, topo, u_ref, g_ref, a_ref, sg_hbm, su_hbm, sd_hbm, eg_hbm, eu_hbm, ed_hbm, out_ref,
               u_all, g_all, x_buf, oht_buf, g_loc, acc_buf, mid_buf, shared_mid, y_buf, s_acc, part, px, ring_in,
               gu_buf, dn_buf, gu_sem, dn_sem,
               agu_send, agu_recv, agg_send, agg_recv, pru_send, pru_recv, prg_send, prg_recv,
               px_send, px_recv, rs_send, rs_recv):
    num_devs, half_steps = topo
    ring_len = num_devs // 2
    me = lax.axis_index(axis)
    ring_pos = me // 2
    core = me % 2
    up_dev = ((ring_pos + 1) % ring_len) * 2 + core
    down_dev = ((ring_pos + ring_len - 1) % ring_len) * 2 + core
    pair_dev = ring_pos * 2 + (1 - core)
    ring_dev = (up_dev, down_dev)
    rows, width = u_ref.shape
    half_rows = rows // 2
    local_experts, _, ff_dim = eg_hbm.shape
    k_chunk = gu_buf.shape[1]
    num_k = width // k_chunk
    num_gu = local_experts * num_k
    gu_slots = gu_buf.shape[0]
    col_chunk = dn_buf.shape[2]
    num_cols = width // col_chunk
    num_dn = num_cols * local_experts
    dn_slots = dn_buf.shape[0]
    slots = x_buf.shape[1] // local_experts
    num_shared_gu = 2 * num_k
    num_shared_dn = 2 * num_cols
    num_pieces = 2 * half_steps - 1

    def gu_copies(j):
        slot = lax.rem(j, gu_slots)
        e = lax.div(j, num_k)
        off = pl.multiple_of(lax.rem(j, num_k) * k_chunk, k_chunk)
        return (
            pltpu.make_async_copy(eg_hbm.at[e, pl.ds(off, k_chunk), :], gu_buf.at[slot, :, pl.ds(0, ff_dim)], gu_sem.at[slot, 0]),
            pltpu.make_async_copy(eu_hbm.at[e, pl.ds(off, k_chunk), :], gu_buf.at[slot, :, pl.ds(ff_dim, ff_dim)], gu_sem.at[slot, 1]),
        )

    def shared_gu_copy(j):
        src = (sg_hbm, su_hbm)[j // num_k]
        slot = (num_gu + j) % gu_slots
        return pltpu.make_async_copy(src.at[pl.ds((j % num_k) * k_chunk, k_chunk), :], gu_buf.at[slot], gu_sem.at[slot, 0])

    def shared_dn_copy(q):
        slot = (num_dn + q) % dn_slots
        rws = pl.ds((q % 2) * ff_dim, ff_dim)
        return pltpu.make_async_copy(sd_hbm.at[rws, pl.ds((q // 2) * col_chunk, col_chunk)], dn_buf.at[slot], dn_sem.at[slot])

    def dn_copy(q):
        slot = lax.rem(q, dn_slots)
        e = lax.rem(q, local_experts)
        off = pl.multiple_of(lax.div(q, local_experts) * col_chunk, col_chunk)
        return pltpu.make_async_copy(ed_hbm.at[e, :, pl.ds(off, col_chunk)], dn_buf.at[slot], dn_sem.at[slot])

    def start_all(copies):
        for cp in copies:
            cp.start()

    def wait_all(copies):
        for cp in copies:
            cp.wait()

    for j in range(gu_slots):
        start_all(gu_copies(j))
    for q in range(dn_slots):
        dn_copy(q).start()

    barrier = pltpu.get_barrier_semaphore()
    for dev in (up_dev, down_dev, pair_dev):
        pl.semaphore_signal(barrier, inc=1, device_id={axis: dev}, device_id_type=MESH)
    pl.semaphore_wait(barrier, 3)

    def piece_rows(direction, p):
        half = p % 2 if direction == 0 else 1 - p % 2
        return pl.ds(half * half_rows, half_rows)

    def held_slot(direction, step):
        return (ring_len - step) % ring_len if direction == 0 else step

    def gather_copies(direction, p, own):
        step = p // 2
        rws = piece_rows(direction, p)
        dst = held_slot(direction, step + 1)
        u_src = u_ref.at[rws] if own else u_all.at[0, held_slot(direction, step), rws]
        g_src = g_ref.at[rws] if own else g_all.at[0, held_slot(direction, step), rws]
        return (
            pltpu.make_async_remote_copy(src_ref=u_src, dst_ref=u_all.at[0, dst, rws], send_sem=agu_send.at[direction, p], recv_sem=agu_recv.at[direction, p], device_id={axis: ring_dev[direction]}, device_id_type=MESH),
            pltpu.make_async_remote_copy(src_ref=g_src, dst_ref=g_all.at[0, dst, rws], send_sem=agg_send.at[direction, p], recv_sem=agg_recv.at[direction, p], device_id={axis: ring_dev[direction]}, device_id_type=MESH),
        )

    def pair_copies(direction, p):
        rws = piece_rows(direction, p)
        slot = held_slot(direction, p // 2 + 1)
        return (
            pltpu.make_async_remote_copy(src_ref=u_all.at[0, slot, rws], dst_ref=u_all.at[1, slot, rws], send_sem=pru_send.at[direction, p], recv_sem=pru_recv.at[direction, p], device_id={axis: pair_dev}, device_id_type=MESH),
            pltpu.make_async_remote_copy(src_ref=g_all.at[0, slot, rws], dst_ref=g_all.at[1, slot, rws], send_sem=prg_send.at[direction, p], recv_sem=prg_recv.at[direction, p], device_id={axis: pair_dev}, device_id_type=MESH),
        )

    pair_own = (
        pltpu.make_async_remote_copy(src_ref=u_ref, dst_ref=u_all.at[1, 0], send_sem=pru_send.at[0, num_pieces], recv_sem=pru_recv.at[0, num_pieces], device_id={axis: pair_dev}, device_id_type=MESH),
        pltpu.make_async_remote_copy(src_ref=g_ref, dst_ref=g_all.at[1, 0], send_sem=prg_send.at[0, num_pieces], recv_sem=prg_recv.at[0, num_pieces], device_id={axis: pair_dev}, device_id_type=MESH),
    )

    for p in range(2):
        for direction in range(2):
            start_all(gather_copies(direction, p, True))
    start_all(pair_own)
    u_all[0, 0] = u_ref[...]
    g_all[0, 0] = g_ref[...]

    def gather_event(p):
        for direction in range(2):
            for cp in gather_copies(direction, p, False):
                cp.wait_recv()

        if p + 2 < num_pieces:
            for direction in range(2):
                start_all(gather_copies(direction, p + 2, False))
        for direction in range(2):
            start_all(pair_copies(direction, p))

    for p in range(num_pieces):
        gather_event(p)
    for direction in range(2):
        for p in range(num_pieces):
            for cp in pair_copies(direction, p):
                cp.wait_recv()
    for cp in pair_own:
        cp.wait_recv()

    total_rows = num_devs * rows
    g_full = g_all[...].reshape(total_rows, g_all.shape[3])
    lanes = g_full.shape[1]
    g_mine = pltpu.roll(g_full, lax.rem(lanes - me * local_experts, lanes), 1)
    g_loc[...] = jnp.maximum(g_mine, 0.0)
    hit = g_mine >= 0.0
    row_i = lax.broadcasted_iota(jnp.int32, (total_rows, total_rows), 0)
    col_i = lax.broadcasted_iota(jnp.int32, (total_rows, total_rows), 1)
    before = jnp.where(col_i < row_i, 1.0, 0.0).astype(jnp.bfloat16)
    rank = jnp.dot(before, jnp.where(hit, 1.0, 0.0).astype(jnp.bfloat16), preferred_element_type=jnp.float32)
    place = jnp.where(hit, rank, -1.0)
    slot_i = lax.broadcasted_iota(jnp.int32, (total_rows, slots), 1).astype(jnp.float32)
    u_rows = u_all[...].reshape(total_rows, width)
    for e in range(local_experts):
        one_hot = jnp.where(slot_i == place[:, e:e + 1], 1.0, 0.0)
        oht_buf[e] = one_hot.astype(jnp.bfloat16)
        pick = one_hot.T.astype(jnp.bfloat16)
        for k in range(num_k):
            x_buf[k, e * slots:(e + 1) * slots] = jnp.dot(pick, u_rows[:, k * k_chunk:(k + 1) * k_chunk], preferred_element_type=jnp.float32).astype(jnp.bfloat16)

    def expert_step(e, carry):
        for k in range(num_k):
            j = e * num_k + k
            slot = lax.rem(j, gu_slots)
            wait_all(gu_copies(j))
            prod = jnp.dot(x_buf[k, pl.ds(pl.multiple_of(e * slots, slots), slots)], gu_buf[slot], preferred_element_type=jnp.float32)
            if k == 0:
                acc_buf[...] = prod
            else:
                acc_buf[...] += prod

            @pl.when(j + gu_slots < num_gu)
            def _():
                start_all(gu_copies(j + gu_slots))

        mid_buf[e] = (jax.nn.silu(acc_buf[:, :ff_dim]) * acc_buf[:, ff_dim:]).astype(jnp.bfloat16)
        return carry

    lax.fori_loop(0, local_experts, expert_step, 0)
    half_cols = col_chunk // 2

    def pair_sum_copy(c):
        return pltpu.make_async_remote_copy(src_ref=part.at[c, 1], dst_ref=px.at[c], send_sem=px_send.at[c], recv_sem=px_recv.at[c], device_id={axis: pair_dev}, device_id_type=MESH)

    def sum_slot(direction, step):
        return half_steps - step if direction == 0 else (half_steps + step) % ring_len

    def ring_copy(c, direction, step):
        slot = sum_slot(direction, step)
        if step == 0:
            cols = pl.ds(direction * half_cols, half_cols)
            src, dst = part.at[c, 0, slot, :, cols], ring_in.at[direction, c, step, :, cols]
        else:
            src, dst = part.at[c, 0, slot], ring_in.at[direction, c, step]
        return pltpu.make_async_remote_copy(src_ref=src, dst_ref=dst, send_sem=rs_send.at[direction, c, step], recv_sem=rs_recv.at[direction, c, step], device_id={axis: ring_dev[direction]}, device_id_type=MESH)

    def column_sums(c):
        for e in range(local_experts):
            q = c * local_experts + e
            dn_copy(q).wait()
            y_buf[e] = jnp.dot(mid_buf[e], dn_buf[q % dn_slots], preferred_element_type=jnp.float32).astype(jnp.bfloat16)
            ahead = q + dn_slots
            if ahead < num_dn:
                dn_copy(ahead).start()
            else:
                if ahead - num_dn < num_shared_gu:
                    shared_gu_copy(ahead - num_dn).start()
                if ahead - num_dn < num_shared_dn:
                    shared_dn_copy(ahead - num_dn).start()
        total = None
        for e in range(local_experts):
            spread = jnp.dot(oht_buf[e], y_buf[e], preferred_element_type=jnp.float32) * g_loc[:, e:e + 1]
            total = spread if total is None else total + spread
        part[c] = total.reshape(2, ring_len, rows, col_chunk)
        pair_sum_copy(c).start()

    def ring_step(c, step):
        if step == 0:
            pair_sum_copy(c).wait_recv()
            part[c, 0, half_steps] += px[c, half_steps]
            for direction in range(2):
                ring_copy(c, direction, 0).start()
            return
        for direction in range(2):
            slot = sum_slot(direction, step)
            ring_copy(c, direction, step - 1).wait_recv()
            if step == 1:
                cols = slice(direction * half_cols, (direction + 1) * half_cols)
                part[c, 0, slot] += px[c, slot]
                part[c, 0, slot, :, cols] += ring_in[direction, c, 0, :, cols]
            elif step < half_steps:
                part[c, 0, slot] += px[c, slot] + ring_in[direction, c, step - 1]
            if step < half_steps:
                ring_copy(c, direction, step).start()
        if step == half_steps:
            part[c, 0, 0] += px[c, 0] + ring_in[0, c, step - 1] + ring_in[1, c, step - 1]

    def shared_gu(j):
        shared_gu_copy(j).wait()
        k = j % num_k
        rws = pl.ds((j // num_k) * rows, rows)
        prod = jnp.dot(u_ref[:, k * k_chunk:(k + 1) * k_chunk], gu_buf[(num_gu + j) % gu_slots], preferred_element_type=jnp.float32)
        if k == 0:
            acc_buf[rws] = prod
        else:
            acc_buf[rws] += prod
        if j == num_shared_gu - 1:
            act = (jax.nn.silu(acc_buf[:rows]) * acc_buf[rows:2 * rows]).astype(jnp.bfloat16)
            for h in range(2):
                shared_mid[h] = act[:, h * ff_dim:(h + 1) * ff_dim]

    def shared_dn(q):
        shared_dn_copy(q).wait()
        cols = slice((q // 2) * col_chunk, (q // 2 + 1) * col_chunk)
        prod = jnp.dot(shared_mid[q % 2], dn_buf[(num_dn + q) % dn_slots], preferred_element_type=jnp.float32)
        if q % 2 == 0:
            s_acc[:, cols] = prod
        else:
            s_acc[:, cols] += prod

    fillers = [functools.partial(shared_gu, j) for j in range(num_shared_gu)] + [functools.partial(shared_dn, q) for q in range(num_shared_dn)]

    for turn in range(num_cols + half_steps + 1):
        if turn < num_cols:
            column_sums(turn)
        for step in range(half_steps + 1):
            c = turn - 1 - step
            if 0 <= c < num_cols:
                ring_step(c, step)
                if turn >= num_cols:
                    for filler in fillers[:2]:
                        filler()
                    fillers = fillers[2:]
    for filler in fillers:
        filler()
    for c in range(num_cols):
        cols = slice(c * col_chunk, (c + 1) * col_chunk)
        out_ref[:, cols] = (a_ref[:, cols].astype(jnp.float32) + s_acc[:, cols] + part[c, 0, 0]).astype(jnp.bfloat16)

    for direction in range(2):
        for p in range(num_pieces):
            for cp in gather_copies(direction, p, p < 2) + pair_copies(direction, p):
                cp.wait_send()
        for c in range(num_cols):
            for step in range(half_steps):
                ring_copy(c, direction, step).wait_send()
    for cp in pair_own:
        cp.wait_send()
    for c in range(num_cols):
        pair_sum_copy(c).wait_send()


def moe_call(axis, num_devs, moe_in, gate_rows, resid_out, shared_gate, shared_up, shared_down, expert_gate, expert_up, expert_down, slots):
    rows, width = moe_in.shape
    local_experts, _, ff_dim = expert_gate.shape
    assert shared_down.shape[0] == 2 * ff_dim
    ring_len = num_devs // 2
    half_steps = ring_len // 2
    k_chunk = min(512, width // 2)
    num_k = width // k_chunk
    gu_slots = min(10, local_experts * num_k)
    num_cols = 4
    col_chunk = width // num_cols
    dn_slots = 10
    num_pieces = 2 * half_steps - 1
    lanes = gate_rows.shape[1]
    f32, bf16 = jnp.float32, jnp.bfloat16
    vmem = pl.BlockSpec(memory_space=pltpu.VMEM)
    anym = pl.BlockSpec(memory_space=pl.ANY)
    dma = pltpu.SemaphoreType.DMA
    return pl.pallas_call(
        functools.partial(moe_kernel, axis, (num_devs, half_steps)),
        name='moe_ring',
        out_shape=jax.ShapeDtypeStruct((rows, width), bf16),
        in_specs=[vmem] * 3 + [anym] * 6,
        out_specs=vmem,
        scratch_shapes=[
            pltpu.VMEM((2, ring_len, rows, width), bf16),
            pltpu.VMEM((2, ring_len, rows, lanes), f32),
            pltpu.VMEM((num_k, local_experts * slots, k_chunk), bf16),
            pltpu.VMEM((local_experts, num_devs * rows, slots), bf16),
            pltpu.VMEM((num_devs * rows, lanes), f32),
            pltpu.VMEM((slots, 2 * ff_dim), f32),
            pltpu.VMEM((local_experts, slots, ff_dim), bf16),
            pltpu.VMEM((2, rows, ff_dim), bf16),
            pltpu.VMEM((local_experts, slots, col_chunk), bf16),
            pltpu.VMEM((rows, width), f32),
            pltpu.VMEM((num_cols, 2, ring_len, rows, col_chunk), f32),
            pltpu.VMEM((num_cols, ring_len, rows, col_chunk), f32),
            pltpu.VMEM((2, num_cols, half_steps, rows, col_chunk), f32),
            pltpu.VMEM((gu_slots, k_chunk, 2 * ff_dim), bf16),
            pltpu.VMEM((dn_slots, ff_dim, col_chunk), bf16),
            dma((gu_slots, 2)), dma((dn_slots,)),
            dma((2, num_pieces)), dma((2, num_pieces)), dma((2, num_pieces)), dma((2, num_pieces)),
            dma((2, num_pieces + 1)), dma((2, num_pieces + 1)), dma((2, num_pieces + 1)), dma((2, num_pieces + 1)),
            dma((num_cols,)), dma((num_cols,)), dma((2, num_cols, half_steps)), dma((2, num_cols, half_steps)),
        ],
        compiler_params=pltpu.CompilerParams(collective_id=0, has_side_effects=True, vmem_limit_bytes=67043328),
    )(moe_in, gate_rows, resid_out, shared_gate, shared_up, shared_down, expert_gate, expert_up, expert_down)


def solution(mesh):
    row_spec = P(('rep', 'dp'))
    full_spec = P()
    expert_spec = P('dp')
    num_devs = mesh.shape['dp']

    def device_step(hidden, ckv_cache, kr_cache, seq_lens, expert_ids, attn_gain, kv_gain, moe_gain, w_q, w_dkv, w_uk, w_uv, w_o, w_router, shared_gate, shared_up, shared_down, expert_gate, expert_up, expert_down):
        capacity = max(2, 2 * hidden.shape[0] * expert_ids.shape[1] // w_router.shape[1])
        slots = -(-capacity * num_devs // 128) * 128
        resid_out, moe_in, gate_rows, ckv_new, kr_new = attn_call(hidden, ckv_cache, kr_cache, seq_lens, expert_ids, attn_gain, kv_gain, moe_gain, w_q, w_dkv, w_uk, w_uv, w_o, w_router)
        layer_out = moe_call('dp', num_devs, moe_in, gate_rows, resid_out, shared_gate, shared_up, shared_down, expert_gate, expert_up, expert_down, slots)
        return layer_out, ckv_new, kr_new

    in_specs = (row_spec,) * 5 + (full_spec,) * 12 + (expert_spec,) * 3
    return jax.shard_map(device_step, mesh=mesh, in_specs=in_specs, out_specs=(row_spec, row_spec, row_spec), check_vma=False)
```

```python
import functools
import math

import jax
import jax.numpy as jnp
from jax import lax
from jax.experimental import pallas as pl
from jax.experimental.pallas import tpu as pltpu
from jax.sharding import PartitionSpec as P

NORM_EPS = 1e-6
ROPE_THETA = 10000.0
MESH = pl.DeviceIdType.MESH


def attn_kernel(dims, lens_smem, ids_ref, hid_ref, ag_ref, kg_ref, mg_ref, wq_hbm, wdkv_hbm, wuk_hbm, wuv_hbm, wo_hbm, wr_ref, ckv_hbm, kr_hbm,
                a_ref, u_ref, g_ref, ckvn_ref, krn_ref,
                wq, wdkv, wuk, wuv, wo, ckv, kr, q_lat, q_rot, o_lat, head_out, gate_t,
                wq_sem, wdkv_sem, wuk_sem, wuv_sem, wo_sem, ckv_sem, kr_sem):
    heads, nope_dim, rope_dim, latent, seq_block = dims
    bf16, f32 = jnp.bfloat16, jnp.float32
    rows, width = hid_ref.shape
    cache_len = ckv_hbm.shape[1]
    head_dim = nope_dim + rope_dim
    v_dim = wuv_hbm.shape[2]
    q_chunks = wq_sem.shape[0]
    q_cols = wq_hbm.shape[1] // q_chunks
    uk_chunks = wuk_sem.shape[0]
    uk_heads = heads // uk_chunks
    o_chunks = wo_sem.shape[0]
    o_rows = wo_hbm.shape[0] // o_chunks
    score_scale = head_dim ** -0.5
    tiles = latent // 128

    wq_cp = [pltpu.make_async_copy(wq_hbm.at[:, pl.ds(i * q_cols, q_cols)], wq.at[i], wq_sem.at[i]) for i in range(q_chunks)]
    wdkv_cp = pltpu.make_async_copy(wdkv_hbm, wdkv, wdkv_sem)
    wuk_cp = [pltpu.make_async_copy(wuk_hbm.at[pl.ds(i * uk_heads, uk_heads)], wuk.at[pl.ds(i * uk_heads, uk_heads)], wuk_sem.at[i]) for i in range(uk_chunks)]
    wuv_cp = pltpu.make_async_copy(wuv_hbm, wuv, wuv_sem)
    wo_cp = [pltpu.make_async_copy(wo_hbm.at[pl.ds(i * o_rows, o_rows)], wo.at[i], wo_sem.at[i]) for i in range(o_chunks)]
    seq_blocks = rows // seq_block
    ckv_cp = [pltpu.make_async_copy(ckv_hbm.at[pl.ds(i * seq_block, seq_block)], ckv.at[pl.ds(i * seq_block, seq_block)], ckv_sem.at[i]) for i in range(seq_blocks)]
    kr_cp = pltpu.make_async_copy(kr_hbm, kr, kr_sem)
    waves = [
        [wdkv_cp, wq_cp[0], wuk_cp[0], wq_cp[1]],
        [wq_cp[2]],
        [wq_cp[3], wuk_cp[1]],
        [kr_cp, ckv_cp[0], ckv_cp[1]],
        [wuv_cp, wo_cp[0]],
        [wo_cp[1], wo_cp[2], wo_cp[3]],
    ]

    def start_wave(i):
        for cp in waves[i]:
            cp.start()

    start_wave(0)

    def norm(vals, gain):
        inv = lax.rsqrt(jnp.mean(vals * vals, axis=-1, keepdims=True) + NORM_EPS)
        return (vals * inv * gain.astype(f32).reshape(1, -1)).astype(bf16)

    def dot_t(left, right):
        return lax.dot_general(left, right, (((1,), (1,)), ((), ())), preferred_element_type=f32)

    hid = hid_ref[...].astype(f32)
    x = norm(hid, ag_ref[...])

    lane = lax.broadcasted_iota(jnp.int32, (rows, 2 * rope_dim), 1)
    pair = (lane % (rope_dim // 2)).astype(f32)
    inv_freq = jnp.exp(pair * (-2.0 / rope_dim * math.log(ROPE_THETA)))
    row = lax.broadcasted_iota(jnp.int32, (rows, 2 * rope_dim), 0)
    lens = jnp.zeros((rows, 2 * rope_dim), jnp.int32)
    for b in range(rows):
        lens = jnp.where(row == b, lens_smem[b], lens)
    angles = lens.astype(f32) * inv_freq
    rope_cos, rope_sin = jnp.cos(angles), jnp.sin(angles)
    first = (lane % rope_dim) < rope_dim // 2

    def rope(vals):
        swapped = jnp.where(first, -pltpu.roll(vals, 2 * rope_dim - rope_dim // 2, 1), pltpu.roll(vals, rope_dim // 2, 1))
        return (vals * rope_cos + swapped * rope_sin).astype(bf16)

    wdkv_cp.wait()
    start_wave(1)
    latent_kv = dot_t(x, wdkv[...])
    ckv_new = norm(latent_kv[:, :latent], kg_ref[...])
    ckvn_ref[...] = ckv_new
    k_part = latent_kv[:, latent:latent + rope_dim]
    kr_new = rope(jnp.concatenate([k_part, k_part], axis=1))
    krn_ref[...] = kr_new[:, :rope_dim]

    for i in range(q_chunks):
        wq_cp[i].wait()
        start_wave(2 + i)
        q_part = jnp.dot(x, wq[i], preferred_element_type=f32).astype(bf16).astype(f32)
        chunk_heads = q_cols // head_dim
        if (i * chunk_heads) % uk_heads == 0:
            wuk_cp[i * chunk_heads // uk_heads].wait()
        for m in range(chunk_heads // 2):
            head = i * chunk_heads + 2 * m
            base = 2 * m * head_dim
            both = jnp.where(lane < rope_dim, q_part[:, base + nope_dim:base + nope_dim + 2 * rope_dim], q_part[:, base + nope_dim + 2 * rope_dim:base + 2 * head_dim])
            turned = rope(both).astype(f32)
            q_rot[pl.ds(head, rows, stride=heads), :] = jnp.where(lane < rope_dim, turned, 0.0)
            q_rot[pl.ds(head + 1, rows, stride=heads), :] = jnp.where(lane < rope_dim, pltpu.roll(turned, rope_dim, 1), 0.0)
            for h in range(2):
                q_nope = q_part[:, base + h * head_dim:base + h * head_dim + nope_dim].astype(bf16)
                lat = jnp.dot(q_nope, wuk[head + h], preferred_element_type=f32).astype(bf16).astype(f32)
                for t in range(tiles):
                    q_lat[t, pl.ds(head + h, rows, stride=heads), :] = lat[:, t * 128:(t + 1) * 128]

    kr_cp.wait()
    block_rows = seq_block * heads
    key_lane = lax.broadcasted_iota(jnp.int32, (heads, cache_len), 1)
    new_lane = lax.broadcasted_iota(jnp.int32, (block_rows, rows), 1)
    new_row = lax.div(lax.broadcasted_iota(jnp.int32, (block_rows, rows), 0), heads)

    for i in range(seq_blocks):
        ckv_cp[i].wait()
        base = i * block_rows
        ql = jnp.concatenate([q_lat[t, base:base + block_rows, :] for t in range(tiles)], axis=1).astype(bf16)
        qr = q_rot[base:base + block_rows, :].astype(bf16)[:, :rope_dim]
        new = (dot_t(ql, ckv_new) + dot_t(qr, kr_new[:, :rope_dim])) * score_scale
        new = jnp.where(new_lane == new_row + i * seq_block, new, -jnp.inf)
        scores = []
        for s in range(seq_block):
            b = i * seq_block + s
            part = slice(s * heads, (s + 1) * heads)
            score = (dot_t(ql[part], ckv[b]) + jnp.dot(qr[part], kr[b], preferred_element_type=f32)) * score_scale
            scores.append(jnp.where(key_lane < lens_smem[b], score, -jnp.inf))
        score = jnp.concatenate(scores, axis=0)
        top = jnp.maximum(jnp.max(score, axis=-1, keepdims=True), jnp.max(new, axis=-1, keepdims=True))
        e_cache, e_new = jnp.exp(score - top), jnp.exp(new - top)
        denom = jnp.sum(e_cache, axis=-1, keepdims=True) + jnp.sum(e_new, axis=-1, keepdims=True)
        p_cache, p_new = (e_cache / denom).astype(bf16), (e_new / denom).astype(bf16)
        from_new = jnp.dot(p_new, ckv_new, preferred_element_type=f32)
        for s in range(seq_block):
            part = slice(s * heads, (s + 1) * heads)
            out = jnp.dot(p_cache[part], ckv[i * seq_block + s], preferred_element_type=f32) + from_new[part]
            out = out.astype(bf16).astype(f32)
            for t in range(tiles):
                o_lat[t, base + s * heads:base + (s + 1) * heads, :] = out[:, t * 128:(t + 1) * 128]

    wuv_cp.wait()
    for h in range(heads):
        lat = jnp.concatenate([o_lat[t, pl.ds(h, rows, stride=heads), :] for t in range(tiles)], axis=1).astype(bf16)
        head_out[:, h * v_dim:(h + 1) * v_dim] = jnp.dot(lat, wuv[h], preferred_element_type=f32).astype(bf16)

    total = hid
    for i in range(o_chunks):
        wo_cp[i].wait()
        total = total + jnp.dot(head_out[:, i * o_rows:(i + 1) * o_rows], wo[i], preferred_element_type=f32)
    resid = total.astype(bf16)
    a_ref[...] = resid
    moe_in = norm(resid.astype(f32), mg_ref[...])
    u_ref[...] = moe_in

    half_rows = rows // 2
    num_experts = wr_ref.shape[0]
    gate_t[...] = jnp.full(gate_t.shape, -1.0, f32)
    for half in range(2):
        logits = dot_t(wr_ref[...], moe_in[half * half_rows:(half + 1) * half_rows])
        top = jnp.max(logits, axis=0, keepdims=True)
        e_log = jnp.exp(logits - top)
        probs = e_log / jnp.sum(e_log, axis=0, keepdims=True)
        expert = lax.broadcasted_iota(jnp.int32, logits.shape, 0)
        ids = ids_ref[:, half * half_rows:(half + 1) * half_rows]
        picked = expert == ids[0:1, :]
        for k in range(1, ids.shape[0]):
            picked = picked | (expert == ids[k:k + 1, :])
        gate_t[half * num_experts:(half + 1) * num_experts, :half_rows] = jnp.where(picked, probs, -1.0)
    g_ref[...] = gate_t[...].T[:half_rows]


def attn_call(hidden, ckv_cache, kr_cache, seq_lens, expert_ids, attn_gain, kv_gain, moe_gain, w_q, w_dkv, w_uk, w_uv, w_o, w_router):
    rows, width = hidden.shape
    heads, nope_dim, latent = w_uk.shape
    v_dim = w_uv.shape[2]
    rope_dim = kr_cache.shape[2]
    cache_len = ckv_cache.shape[1]
    seq_block, q_chunks, uk_chunks, o_chunks = rows // 2, 4, 2, 4
    bf16, f32 = jnp.bfloat16, jnp.float32
    vmem = pl.BlockSpec(memory_space=pltpu.VMEM)
    anym = pl.BlockSpec(memory_space=pl.ANY)
    smem = pl.BlockSpec(memory_space=pltpu.SMEM)
    dma = pltpu.SemaphoreType.DMA
    shape = jax.ShapeDtypeStruct
    return pl.pallas_call(
        functools.partial(attn_kernel, (heads, nope_dim, rope_dim, latent, seq_block)),
        name='attention',
        out_shape=(shape((rows, width), bf16), shape((rows, width), bf16), shape((rows // 2, 2 * w_router.shape[1]), f32), shape((rows, latent), bf16), shape((rows, rope_dim), bf16)),
        in_specs=[smem] + [vmem] * 5 + [anym] * 5 + [vmem] + [anym] * 2,
        out_specs=(vmem,) * 5,
        scratch_shapes=[
            pltpu.VMEM((q_chunks, width, w_q.shape[1] // q_chunks), bf16),
            pltpu.VMEM((w_dkv.shape[1], width), bf16),
            pltpu.VMEM(w_uk.shape, bf16),
            pltpu.VMEM(w_uv.shape, bf16),
            pltpu.VMEM((o_chunks, w_o.shape[0] // o_chunks, width), bf16),
            pltpu.VMEM((rows, cache_len, latent), bf16),
            pltpu.VMEM((rows, rope_dim, cache_len), bf16),
            pltpu.VMEM((latent // 128, rows * heads, 128), f32),
            pltpu.VMEM((rows * heads, 2 * rope_dim), f32),
            pltpu.VMEM((latent // 128, rows * heads, 128), f32),
            pltpu.VMEM((rows, heads * v_dim), bf16),
            pltpu.VMEM((2 * w_router.shape[1], 128), f32),
            dma((q_chunks,)), dma, dma((uk_chunks,)), dma, dma((o_chunks,)), dma((rows // seq_block,)), dma,
        ],
        compiler_params=pltpu.CompilerParams(vmem_limit_bytes=60000000),
    )(seq_lens, expert_ids.T, hidden, attn_gain, kv_gain, moe_gain,
      w_q, w_dkv.T, w_uk, w_uv, w_o, w_router.T, ckv_cache, kr_cache.transpose(0, 2, 1))


def moe_kernel(axis, topo, u_ref, g_ref, a_ref, sg_hbm, su_hbm, sd_hbm, eg_hbm, eu_hbm, ed_hbm, out_ref,
               u_all, g_all, x_buf, oht_buf, g_loc, acc_buf, mid_buf, shared_mid, y_buf, s_acc, part, px, ring_in,
               gu_buf, dn_buf, gu_sem, dn_sem,
               agu_send, agu_recv, agg_send, agg_recv, pru_send, pru_recv, prg_send, prg_recv,
               px_send, px_recv, rs_send, rs_recv):
    num_devs, half_steps = topo
    ring_len = num_devs // 2
    me = lax.axis_index(axis)
    ring_pos = me // 2
    core = me % 2
    up_dev = ((ring_pos + 1) % ring_len) * 2 + core
    down_dev = ((ring_pos + ring_len - 1) % ring_len) * 2 + core
    pair_dev = ring_pos * 2 + (1 - core)
    ring_dev = (up_dev, down_dev)
    rows, width = u_ref.shape
    half_rows = rows // 2
    local_experts, _, ff_dim = eg_hbm.shape
    k_chunk = gu_buf.shape[1]
    num_k = width // k_chunk
    num_gu = local_experts * num_k
    gu_slots = gu_buf.shape[0]
    col_chunk = dn_buf.shape[2]
    num_cols = width // col_chunk
    num_dn = num_cols * local_experts
    dn_slots = dn_buf.shape[0]
    slots = x_buf.shape[1] // local_experts
    num_shared_gu = 2 * num_k
    num_shared_dn = 2 * num_cols
    half_width = width // 2
    num_pieces = 4 * half_steps - 2

    def gu_copies(j):
        slot = lax.rem(j, gu_slots)
        e = lax.div(j, num_k)
        off = pl.multiple_of(lax.rem(j, num_k) * k_chunk, k_chunk)
        return (
            pltpu.make_async_copy(eg_hbm.at[e, pl.ds(off, k_chunk), :], gu_buf.at[slot, :, pl.ds(0, ff_dim)], gu_sem.at[slot, 0]),
            pltpu.make_async_copy(eu_hbm.at[e, pl.ds(off, k_chunk), :], gu_buf.at[slot, :, pl.ds(ff_dim, ff_dim)], gu_sem.at[slot, 1]),
        )

    def shared_gu_copy(j):
        src = (sg_hbm, su_hbm)[j // num_k]
        slot = (num_gu + j) % gu_slots
        return pltpu.make_async_copy(src.at[pl.ds((j % num_k) * k_chunk, k_chunk), :], gu_buf.at[slot], gu_sem.at[slot, 0])

    def shared_dn_copy(q):
        slot = (num_dn + q) % dn_slots
        rws = pl.ds((q % 2) * ff_dim, ff_dim)
        return pltpu.make_async_copy(sd_hbm.at[rws, pl.ds((q // 2) * col_chunk, col_chunk)], dn_buf.at[slot], dn_sem.at[slot])

    def dn_copy(q):
        slot = lax.rem(q, dn_slots)
        e = lax.rem(q, local_experts)
        off = pl.multiple_of(lax.div(q, local_experts) * col_chunk, col_chunk)
        return pltpu.make_async_copy(ed_hbm.at[e, :, pl.ds(off, col_chunk)], dn_buf.at[slot], dn_sem.at[slot])

    def start_all(copies):
        for cp in copies:
            cp.start()

    def wait_all(copies):
        for cp in copies:
            cp.wait()

    for j in range(gu_slots):
        start_all(gu_copies(j))
    for q in range(dn_slots):
        dn_copy(q).start()

    barrier = pltpu.get_barrier_semaphore()
    for dev in (up_dev, down_dev, pair_dev):
        pl.semaphore_signal(barrier, inc=1, device_id={axis: dev}, device_id_type=MESH)
    pl.semaphore_wait(barrier, 3)

    def piece_part(direction, p):
        half = p % 4 // 2 if direction == 0 else 1 - p % 4 // 2
        return pl.ds(half * half_rows, half_rows), pl.ds(p % 2 * half_width, half_width)

    def held_slot(direction, step):
        return (ring_len - step) % ring_len if direction == 0 else step

    def gather_copy(direction, p):
        step = p // 4
        part_of = piece_part(direction, p)
        u_src = u_ref.at[part_of] if step == 0 else u_all.at[(0, held_slot(direction, step)) + part_of]
        return pltpu.make_async_remote_copy(src_ref=u_src, dst_ref=u_all.at[(0, held_slot(direction, step + 1)) + part_of], send_sem=agu_send.at[direction, p], recv_sem=agu_recv.at[direction, p], device_id={axis: ring_dev[direction]}, device_id_type=MESH)

    def gate_copy(direction, step):
        g_src = g_ref if step == 0 else g_all.at[0, held_slot(direction, step)]
        return pltpu.make_async_remote_copy(src_ref=g_src, dst_ref=g_all.at[0, held_slot(direction, step + 1)], send_sem=agg_send.at[direction, step], recv_sem=agg_recv.at[direction, step], device_id={axis: ring_dev[direction]}, device_id_type=MESH)

    def pair_copy(direction, p):
        piece = (held_slot(direction, p // 4 + 1),) + piece_part(direction, p)
        return pltpu.make_async_remote_copy(src_ref=u_all.at[(0,) + piece], dst_ref=u_all.at[(1,) + piece], send_sem=pru_send.at[direction, p], recv_sem=pru_recv.at[direction, p], device_id={axis: pair_dev}, device_id_type=MESH)

    def pair_gate_copy(direction, step):
        slot = held_slot(direction, step + 1)
        return pltpu.make_async_remote_copy(src_ref=g_all.at[0, slot], dst_ref=g_all.at[1, slot], send_sem=prg_send.at[direction, step], recv_sem=prg_recv.at[direction, step], device_id={axis: pair_dev}, device_id_type=MESH)

    pair_own = (
        pltpu.make_async_remote_copy(src_ref=u_ref, dst_ref=u_all.at[1, 0], send_sem=pru_send.at[0, num_pieces], recv_sem=pru_recv.at[0, num_pieces], device_id={axis: pair_dev}, device_id_type=MESH),
        pltpu.make_async_remote_copy(src_ref=g_ref, dst_ref=g_all.at[1, 0], send_sem=prg_send.at[0, half_steps], recv_sem=prg_recv.at[0, half_steps], device_id={axis: pair_dev}, device_id_type=MESH),
    )
    gate_steps = (half_steps, half_steps - 1)

    for p in range(4):
        for direction in range(2):
            if p == 0:
                gate_copy(direction, 0).start()
            gather_copy(direction, p).start()
    start_all(pair_own)
    u_all[0, 0] = u_ref[...]
    g_all[0, 0] = g_ref[...]

    for p in range(num_pieces):
        for direction in range(2):
            step = p // 4
            if p % 4 == 0 and step < gate_steps[direction]:
                gate_copy(direction, step).wait_recv()
                if step + 1 < gate_steps[direction]:
                    gate_copy(direction, step + 1).start()
                pair_gate_copy(direction, step).start()
            gather_copy(direction, p).wait_recv()
            if p + 4 < num_pieces:
                gather_copy(direction, p + 4).start()
            pair_copy(direction, p).start()
    for direction in range(2):
        for step in range(gate_steps[direction]):
            pair_gate_copy(direction, step).wait_recv()
        for p in range(num_pieces):
            pair_copy(direction, p).wait_recv()
    for cp in pair_own:
        cp.wait_recv()

    total_rows = num_devs * rows
    lanes = g_all.shape[3]
    packed = g_all[...].reshape(total_rows // 2, lanes)
    low_half = lax.broadcasted_iota(jnp.int32, packed.shape, 1) < lanes // 2
    halves = [jnp.where(low_half, rows_of, -1.0).reshape(num_devs, half_rows, lanes) for rows_of in (packed, pltpu.roll(packed, lanes // 2, 1))]
    g_full = jnp.concatenate(halves, axis=1).reshape(total_rows, lanes)
    g_mine = pltpu.roll(g_full, lax.rem(lanes - me * local_experts, lanes), 1)
    g_loc[...] = jnp.maximum(g_mine, 0.0)
    hit = g_mine >= 0.0
    row_i = lax.broadcasted_iota(jnp.int32, (total_rows, total_rows), 0)
    col_i = lax.broadcasted_iota(jnp.int32, (total_rows, total_rows), 1)
    before = jnp.where(col_i < row_i, 1.0, 0.0).astype(jnp.bfloat16)
    rank = jnp.dot(before, jnp.where(hit, 1.0, 0.0).astype(jnp.bfloat16), preferred_element_type=jnp.float32)
    place = jnp.where(hit, rank, -1.0)
    slot_i = lax.broadcasted_iota(jnp.int32, (total_rows, slots), 1).astype(jnp.float32)
    u_rows = u_all[...].reshape(total_rows, width)
    for e in range(local_experts):
        one_hot = jnp.where(slot_i == place[:, e:e + 1], 1.0, 0.0)
        oht_buf[e] = one_hot.astype(jnp.bfloat16)
        pick = one_hot.T.astype(jnp.bfloat16)
        for k in range(num_k):
            x_buf[k, e * slots:(e + 1) * slots] = jnp.dot(pick, u_rows[:, k * k_chunk:(k + 1) * k_chunk], preferred_element_type=jnp.float32).astype(jnp.bfloat16)

    def expert_step(e, carry):
        for k in range(num_k):
            j = e * num_k + k
            slot = lax.rem(j, gu_slots)
            wait_all(gu_copies(j))
            prod = jnp.dot(x_buf[k, pl.ds(pl.multiple_of(e * slots, slots), slots)], gu_buf[slot], preferred_element_type=jnp.float32)
            if k == 0:
                acc_buf[...] = prod
            else:
                acc_buf[...] += prod

            @pl.when(j + gu_slots < num_gu)
            def _():
                start_all(gu_copies(j + gu_slots))

        mid_buf[e] = (jax.nn.silu(acc_buf[:, :ff_dim]) * acc_buf[:, ff_dim:]).astype(jnp.bfloat16)
        return carry

    lax.fori_loop(0, local_experts, expert_step, 0)
    half_cols = col_chunk // 2

    def pair_sum_copy(c):
        return pltpu.make_async_remote_copy(src_ref=part.at[c, 1], dst_ref=px.at[c], send_sem=px_send.at[c], recv_sem=px_recv.at[c], device_id={axis: pair_dev}, device_id_type=MESH)

    def sum_slot(direction, step):
        return half_steps - step if direction == 0 else (half_steps + step) % ring_len

    def ring_copy(c, direction, step):
        slot = sum_slot(direction, step)
        if step == 0:
            cols = pl.ds(direction * half_cols, half_cols)
            src, dst = part.at[c, 0, slot, :, cols], ring_in.at[direction, c, step, :, cols]
        else:
            src, dst = part.at[c, 0, slot], ring_in.at[direction, c, step]
        return pltpu.make_async_remote_copy(src_ref=src, dst_ref=dst, send_sem=rs_send.at[direction, c, step], recv_sem=rs_recv.at[direction, c, step], device_id={axis: ring_dev[direction]}, device_id_type=MESH)

    def column_sums(c):
        for e in range(local_experts):
            q = c * local_experts + e
            dn_copy(q).wait()
            y_buf[e] = jnp.dot(mid_buf[e], dn_buf[q % dn_slots], preferred_element_type=jnp.float32).astype(jnp.bfloat16)
            ahead = q + dn_slots
            if ahead < num_dn:
                dn_copy(ahead).start()
            elif ahead - num_dn < num_shared_dn:
                shared_dn_copy(ahead - num_dn).start()
        for j in range(c * num_shared_gu // num_cols, (c + 1) * num_shared_gu // num_cols):
            shared_gu_copy(j).start()
        if c >= 1:
            ring_step(c - 1, 0)
        total = None
        for e in range(local_experts):
            spread = jnp.dot(oht_buf[e], y_buf[e], preferred_element_type=jnp.float32) * g_loc[:, e:e + 1]
            total = spread if total is None else total + spread
        part[c] = total.reshape(2, ring_len, rows, col_chunk)
        pair_sum_copy(c).start()

    def ring_step(c, step):
        if step == 0:
            pair_sum_copy(c).wait_recv()
            part[c, 0, half_steps] += px[c, half_steps]
            for direction in range(2):
                ring_copy(c, direction, 0).start()
            return
        for direction in range(2):
            slot = sum_slot(direction, step)
            ring_copy(c, direction, step - 1).wait_recv()
            if step == 1:
                cols = slice(direction * half_cols, (direction + 1) * half_cols)
                part[c, 0, slot] += px[c, slot]
                part[c, 0, slot, :, cols] += ring_in[direction, c, 0, :, cols]
            elif step < half_steps:
                part[c, 0, slot] += px[c, slot] + ring_in[direction, c, step - 1]
            if step < half_steps:
                ring_copy(c, direction, step).start()
        if step == half_steps:
            part[c, 0, 0] += px[c, 0] + ring_in[0, c, step - 1] + ring_in[1, c, step - 1]

    def shared_gu(j):
        shared_gu_copy(j).wait()
        k = j % num_k
        rws = pl.ds((j // num_k) * rows, rows)
        prod = jnp.dot(u_ref[:, k * k_chunk:(k + 1) * k_chunk], gu_buf[(num_gu + j) % gu_slots], preferred_element_type=jnp.float32)
        if k == 0:
            acc_buf[rws] = prod
        else:
            acc_buf[rws] += prod
        if j == num_shared_gu - 1:
            act = (jax.nn.silu(acc_buf[:rows]) * acc_buf[rows:2 * rows]).astype(jnp.bfloat16)
            for h in range(2):
                shared_mid[h] = act[:, h * ff_dim:(h + 1) * ff_dim]

    def shared_dn(q):
        shared_dn_copy(q).wait()
        cols = slice((q // 2) * col_chunk, (q // 2 + 1) * col_chunk)
        prod = jnp.dot(shared_mid[q % 2], dn_buf[(num_dn + q) % dn_slots], preferred_element_type=jnp.float32)
        if q % 2 == 0:
            s_acc[:, cols] = prod
        else:
            s_acc[:, cols] += prod

    fillers = [functools.partial(shared_gu, j) for j in range(num_shared_gu)] + [functools.partial(shared_dn, q) for q in range(num_shared_dn)]

    for turn in range(num_cols + half_steps + 1):
        if turn < num_cols:
            column_sums(turn)
        for step in range(half_steps + 1):
            c = turn - 1 - step
            if 0 <= c < num_cols:
                if step > 0 or turn >= num_cols:
                    ring_step(c, step)
                run = 2 if turn >= num_cols else 0
                for filler in fillers[:run]:
                    filler()
                fillers = fillers[run:]
    for filler in fillers:
        filler()
    for c in range(num_cols):
        cols = slice(c * col_chunk, (c + 1) * col_chunk)
        out_ref[:, cols] = (a_ref[:, cols].astype(jnp.float32) + s_acc[:, cols] + part[c, 0, 0]).astype(jnp.bfloat16)

    for direction in range(2):
        for p in range(num_pieces):
            gather_copy(direction, p).wait_send()
            pair_copy(direction, p).wait_send()
        for step in range(gate_steps[direction]):
            gate_copy(direction, step).wait_send()
            pair_gate_copy(direction, step).wait_send()
        for c in range(num_cols):
            for step in range(half_steps):
                ring_copy(c, direction, step).wait_send()
    for cp in pair_own:
        cp.wait_send()
    for c in range(num_cols):
        pair_sum_copy(c).wait_send()


def moe_call(axis, num_devs, moe_in, gate_rows, resid_out, shared_gate, shared_up, shared_down, expert_gate, expert_up, expert_down, slots):
    rows, width = moe_in.shape
    local_experts, _, ff_dim = expert_gate.shape
    assert shared_down.shape[0] == 2 * ff_dim
    ring_len = num_devs // 2
    half_steps = ring_len // 2
    k_chunk = min(512, width // 2)
    num_k = width // k_chunk
    gu_slots = min(10, local_experts * num_k)
    num_cols = 4
    col_chunk = width // num_cols
    dn_slots = 10
    num_pieces = 4 * half_steps - 2
    lanes = gate_rows.shape[1]
    f32, bf16 = jnp.float32, jnp.bfloat16
    vmem = pl.BlockSpec(memory_space=pltpu.VMEM)
    anym = pl.BlockSpec(memory_space=pl.ANY)
    dma = pltpu.SemaphoreType.DMA
    return pl.pallas_call(
        functools.partial(moe_kernel, axis, (num_devs, half_steps)),
        name='moe_ring',
        out_shape=jax.ShapeDtypeStruct((rows, width), bf16),
        in_specs=[vmem] * 3 + [anym] * 6,
        out_specs=vmem,
        scratch_shapes=[
            pltpu.VMEM((2, ring_len, rows, width), bf16),
            pltpu.VMEM((2, ring_len, rows // 2, lanes), f32),
            pltpu.VMEM((num_k, local_experts * slots, k_chunk), bf16),
            pltpu.VMEM((local_experts, num_devs * rows, slots), bf16),
            pltpu.VMEM((num_devs * rows, lanes), f32),
            pltpu.VMEM((slots, 2 * ff_dim), f32),
            pltpu.VMEM((local_experts, slots, ff_dim), bf16),
            pltpu.VMEM((2, rows, ff_dim), bf16),
            pltpu.VMEM((local_experts, slots, col_chunk), bf16),
            pltpu.VMEM((rows, width), f32),
            pltpu.VMEM((num_cols, 2, ring_len, rows, col_chunk), f32),
            pltpu.VMEM((num_cols, ring_len, rows, col_chunk), f32),
            pltpu.VMEM((2, num_cols, half_steps, rows, col_chunk), f32),
            pltpu.VMEM((gu_slots, k_chunk, 2 * ff_dim), bf16),
            pltpu.VMEM((dn_slots, ff_dim, col_chunk), bf16),
            dma((gu_slots, 2)), dma((dn_slots,)),
            dma((2, num_pieces)), dma((2, num_pieces)), dma((2, half_steps)), dma((2, half_steps)),
            dma((2, num_pieces + 1)), dma((2, num_pieces + 1)), dma((2, half_steps + 1)), dma((2, half_steps + 1)),
            dma((num_cols,)), dma((num_cols,)), dma((2, num_cols, half_steps)), dma((2, num_cols, half_steps)),
        ],
        compiler_params=pltpu.CompilerParams(collective_id=0, has_side_effects=True, vmem_limit_bytes=67043328),
    )(moe_in, gate_rows, resid_out, shared_gate, shared_up, shared_down, expert_gate, expert_up, expert_down)


def solution(mesh):
    row_spec = P(('rep', 'dp'))
    full_spec = P()
    expert_spec = P('dp')
    num_devs = mesh.shape['dp']

    def device_step(hidden, ckv_cache, kr_cache, seq_lens, expert_ids, attn_gain, kv_gain, moe_gain, w_q, w_dkv, w_uk, w_uv, w_o, w_router, shared_gate, shared_up, shared_down, expert_gate, expert_up, expert_down):
        capacity = max(2, 2 * hidden.shape[0] * expert_ids.shape[1] // w_router.shape[1])
        slots = -(-capacity * num_devs // 128) * 128
        resid_out, moe_in, gate_rows, ckv_new, kr_new = attn_call(hidden, ckv_cache, kr_cache, seq_lens, expert_ids, attn_gain, kv_gain, moe_gain, w_q, w_dkv, w_uk, w_uv, w_o, w_router)
        layer_out = moe_call('dp', num_devs, moe_in, gate_rows, resid_out, shared_gate, shared_up, shared_down, expert_gate, expert_up, expert_down, slots)
        return layer_out, ckv_new, kr_new

    in_specs = (row_spec,) * 5 + (full_spec,) * 12 + (expert_spec,) * 3
    return jax.shard_map(device_step, mesh=mesh, in_specs=in_specs, out_specs=(row_spec, row_spec, row_spec), check_vma=False)
```

```python
import functools
import math

import jax
import jax.numpy as jnp
from jax import lax
from jax.experimental import pallas as pl
from jax.experimental.pallas import tpu as pltpu
from jax.sharding import PartitionSpec as P

NORM_EPS = 1e-6
ROPE_THETA = 10000.0
MESH = pl.DeviceIdType.MESH


def attn_kernel(dims, lens_smem, hid_ref, ag_ref, kg_ref, mg_ref, wq_hbm, wdkv_hbm, wuk_hbm, wuv_hbm, wo_hbm, ckv_hbm, kr_hbm,
                a_ref, u_ref, ckvn_ref, krn_ref,
                wq, wdkv, wuk, wuv, wo, ckv, kr, q_lat, q_rot, o_lat, head_out,
                wq_sem, wdkv_sem, wuk_sem, wuv_sem, wo_sem, ckv_sem, kr_sem):
    heads, nope_dim, rope_dim, latent, seq_block = dims
    bf16, f32 = jnp.bfloat16, jnp.float32
    rows, width = hid_ref.shape
    cache_len = ckv_hbm.shape[1]
    head_dim = nope_dim + rope_dim
    v_dim = wuv_hbm.shape[2]
    q_chunks = wq_sem.shape[0]
    q_cols = wq_hbm.shape[1] // q_chunks
    uk_chunks = wuk_sem.shape[0]
    uk_heads = heads // uk_chunks
    o_chunks = wo_sem.shape[0]
    o_rows = wo_hbm.shape[0] // o_chunks
    score_scale = head_dim ** -0.5
    tiles = latent // 128

    wq_cp = [pltpu.make_async_copy(wq_hbm.at[:, pl.ds(i * q_cols, q_cols)], wq.at[i], wq_sem.at[i]) for i in range(q_chunks)]
    wdkv_cp = pltpu.make_async_copy(wdkv_hbm, wdkv, wdkv_sem)
    wuk_cp = [pltpu.make_async_copy(wuk_hbm.at[pl.ds(i * uk_heads, uk_heads)], wuk.at[pl.ds(i * uk_heads, uk_heads)], wuk_sem.at[i]) for i in range(uk_chunks)]
    wuv_cp = pltpu.make_async_copy(wuv_hbm, wuv, wuv_sem)
    wo_cp = [pltpu.make_async_copy(wo_hbm.at[pl.ds(i * o_rows, o_rows)], wo.at[i], wo_sem.at[i]) for i in range(o_chunks)]
    seq_blocks = rows // seq_block
    ckv_cp = [pltpu.make_async_copy(ckv_hbm.at[pl.ds(i * seq_block, seq_block)], ckv.at[pl.ds(i * seq_block, seq_block)], ckv_sem.at[i]) for i in range(seq_blocks)]
    kr_cp = pltpu.make_async_copy(kr_hbm, kr, kr_sem)
    waves = [
        [wdkv_cp, wq_cp[0], wuk_cp[0], wq_cp[1]],
        [wq_cp[2]],
        [wq_cp[3], wuk_cp[1]],
        [kr_cp, ckv_cp[0], ckv_cp[1]],
        [wuv_cp, wo_cp[0]],
        [wo_cp[1], wo_cp[2], wo_cp[3]],
    ]

    def start_wave(i):
        for cp in waves[i]:
            cp.start()

    start_wave(0)

    def norm(vals, gain):
        inv = lax.rsqrt(jnp.mean(vals * vals, axis=-1, keepdims=True) + NORM_EPS)
        return (vals * inv * gain.astype(f32).reshape(1, -1)).astype(bf16)

    def dot_t(left, right):
        return lax.dot_general(left, right, (((1,), (1,)), ((), ())), preferred_element_type=f32)

    hid = hid_ref[...].astype(f32)
    x = norm(hid, ag_ref[...])

    lane = lax.broadcasted_iota(jnp.int32, (rows, 2 * rope_dim), 1)
    pair = (lane % (rope_dim // 2)).astype(f32)
    inv_freq = jnp.exp(pair * (-2.0 / rope_dim * math.log(ROPE_THETA)))
    row = lax.broadcasted_iota(jnp.int32, (rows, 2 * rope_dim), 0)
    lens = jnp.zeros((rows, 2 * rope_dim), jnp.int32)
    for b in range(rows):
        lens = jnp.where(row == b, lens_smem[b], lens)
    angles = lens.astype(f32) * inv_freq
    rope_cos, rope_sin = jnp.cos(angles), jnp.sin(angles)
    first = (lane % rope_dim) < rope_dim // 2

    def rope(vals):
        swapped = jnp.where(first, -pltpu.roll(vals, 2 * rope_dim - rope_dim // 2, 1), pltpu.roll(vals, rope_dim // 2, 1))
        return (vals * rope_cos + swapped * rope_sin).astype(bf16)

    wdkv_cp.wait()
    start_wave(1)
    latent_kv = dot_t(x, wdkv[...])
    ckv_new = norm(latent_kv[:, :latent], kg_ref[...])
    ckvn_ref[...] = ckv_new
    k_part = latent_kv[:, latent:latent + rope_dim]
    kr_new = rope(jnp.concatenate([k_part, k_part], axis=1))
    krn_ref[...] = kr_new[:, :rope_dim]

    for i in range(q_chunks):
        wq_cp[i].wait()
        start_wave(2 + i)
        q_part = jnp.dot(x, wq[i], preferred_element_type=f32).astype(bf16).astype(f32)
        chunk_heads = q_cols // head_dim
        if (i * chunk_heads) % uk_heads == 0:
            wuk_cp[i * chunk_heads // uk_heads].wait()
        for m in range(chunk_heads // 2):
            head = i * chunk_heads + 2 * m
            base = 2 * m * head_dim
            both = jnp.where(lane < rope_dim, q_part[:, base + nope_dim:base + nope_dim + 2 * rope_dim], q_part[:, base + nope_dim + 2 * rope_dim:base + 2 * head_dim])
            turned = rope(both).astype(f32)
            q_rot[pl.ds(head, rows, stride=heads), :] = jnp.where(lane < rope_dim, turned, 0.0)
            q_rot[pl.ds(head + 1, rows, stride=heads), :] = jnp.where(lane < rope_dim, pltpu.roll(turned, rope_dim, 1), 0.0)
            for h in range(2):
                q_nope = q_part[:, base + h * head_dim:base + h * head_dim + nope_dim].astype(bf16)
                lat = jnp.dot(q_nope, wuk[head + h], preferred_element_type=f32).astype(bf16).astype(f32)
                for t in range(tiles):
                    q_lat[t, pl.ds(head + h, rows, stride=heads), :] = lat[:, t * 128:(t + 1) * 128]

    kr_cp.wait()
    block_rows = seq_block * heads
    key_lane = lax.broadcasted_iota(jnp.int32, (heads, cache_len), 1)
    new_lane = lax.broadcasted_iota(jnp.int32, (block_rows, rows), 1)
    new_row = lax.div(lax.broadcasted_iota(jnp.int32, (block_rows, rows), 0), heads)

    for i in range(seq_blocks):
        ckv_cp[i].wait()
        base = i * block_rows
        ql = jnp.concatenate([q_lat[t, base:base + block_rows, :] for t in range(tiles)], axis=1).astype(bf16)
        qr = q_rot[base:base + block_rows, :].astype(bf16)[:, :rope_dim]
        new = (dot_t(ql, ckv_new) + dot_t(qr, kr_new[:, :rope_dim])) * score_scale
        new = jnp.where(new_lane == new_row + i * seq_block, new, -jnp.inf)
        scores = []
        for s in range(seq_block):
            b = i * seq_block + s
            part = slice(s * heads, (s + 1) * heads)
            score = (dot_t(ql[part], ckv[b]) + jnp.dot(qr[part], kr[b], preferred_element_type=f32)) * score_scale
            scores.append(jnp.where(key_lane < lens_smem[b], score, -jnp.inf))
        score = jnp.concatenate(scores, axis=0)
        top = jnp.maximum(jnp.max(score, axis=-1, keepdims=True), jnp.max(new, axis=-1, keepdims=True))
        e_cache, e_new = jnp.exp(score - top), jnp.exp(new - top)
        denom = jnp.sum(e_cache, axis=-1, keepdims=True) + jnp.sum(e_new, axis=-1, keepdims=True)
        p_cache, p_new = (e_cache / denom).astype(bf16), (e_new / denom).astype(bf16)
        from_new = jnp.dot(p_new, ckv_new, preferred_element_type=f32)
        for s in range(seq_block):
            part = slice(s * heads, (s + 1) * heads)
            out = jnp.dot(p_cache[part], ckv[i * seq_block + s], preferred_element_type=f32) + from_new[part]
            out = out.astype(bf16).astype(f32)
            for t in range(tiles):
                o_lat[t, base + s * heads:base + (s + 1) * heads, :] = out[:, t * 128:(t + 1) * 128]

    wuv_cp.wait()
    for h in range(heads):
        lat = jnp.concatenate([o_lat[t, pl.ds(h, rows, stride=heads), :] for t in range(tiles)], axis=1).astype(bf16)
        head_out[:, h * v_dim:(h + 1) * v_dim] = jnp.dot(lat, wuv[h], preferred_element_type=f32).astype(bf16)

    total = hid
    for i in range(o_chunks):
        wo_cp[i].wait()
        total = total + jnp.dot(head_out[:, i * o_rows:(i + 1) * o_rows], wo[i], preferred_element_type=f32)
    resid = total.astype(bf16)
    a_ref[...] = resid
    moe_in = norm(resid.astype(f32), mg_ref[...])
    u_ref[...] = moe_in


def attn_call(hidden, ckv_cache, kr_cache, seq_lens, attn_gain, kv_gain, moe_gain, w_q, w_dkv, w_uk, w_uv, w_o):
    rows, width = hidden.shape
    heads, nope_dim, latent = w_uk.shape
    v_dim = w_uv.shape[2]
    rope_dim = kr_cache.shape[2]
    cache_len = ckv_cache.shape[1]
    seq_block, q_chunks, uk_chunks, o_chunks = rows // 2, 4, 2, 4
    bf16, f32 = jnp.bfloat16, jnp.float32
    vmem = pl.BlockSpec(memory_space=pltpu.VMEM)
    anym = pl.BlockSpec(memory_space=pl.ANY)
    smem = pl.BlockSpec(memory_space=pltpu.SMEM)
    dma = pltpu.SemaphoreType.DMA
    shape = jax.ShapeDtypeStruct
    return pl.pallas_call(
        functools.partial(attn_kernel, (heads, nope_dim, rope_dim, latent, seq_block)),
        name='attention',
        out_shape=(shape((rows, width), bf16), shape((rows, width), bf16), shape((rows, latent), bf16), shape((rows, rope_dim), bf16)),
        in_specs=[smem] + [vmem] * 4 + [anym] * 7,
        out_specs=(vmem,) * 4,
        scratch_shapes=[
            pltpu.VMEM((q_chunks, width, w_q.shape[1] // q_chunks), bf16),
            pltpu.VMEM((w_dkv.shape[1], width), bf16),
            pltpu.VMEM(w_uk.shape, bf16),
            pltpu.VMEM(w_uv.shape, bf16),
            pltpu.VMEM((o_chunks, w_o.shape[0] // o_chunks, width), bf16),
            pltpu.VMEM((rows, cache_len, latent), bf16),
            pltpu.VMEM((rows, rope_dim, cache_len), bf16),
            pltpu.VMEM((latent // 128, rows * heads, 128), f32),
            pltpu.VMEM((rows * heads, 2 * rope_dim), f32),
            pltpu.VMEM((latent // 128, rows * heads, 128), f32),
            pltpu.VMEM((rows, heads * v_dim), bf16),
            dma((q_chunks,)), dma, dma((uk_chunks,)), dma, dma((o_chunks,)), dma((rows // seq_block,)), dma,
        ],
        compiler_params=pltpu.CompilerParams(vmem_limit_bytes=60000000),
    )(seq_lens, hidden, attn_gain, kv_gain, moe_gain,
      w_q, w_dkv.T, w_uk, w_uv, w_o, ckv_cache, kr_cache.transpose(0, 2, 1))


def moe_kernel(axis, topo, u_ref, a_ref, wr_ref, ids_ref, sg_hbm, su_hbm, sd_hbm, eg_hbm, eu_hbm, ed_hbm, out_ref,
               gate_t, g_ref, u_all, g_all, x_buf, oht_buf, g_loc, acc_buf, mid_buf, shared_mid, y_buf, s_acc, part, px, ring_in,
               gu_buf, dn_buf, gu_sem, dn_sem,
               agu_send, agu_recv, agg_send, agg_recv, pru_send, pru_recv, prg_send, prg_recv,
               px_send, px_recv, rs_send, rs_recv):
    num_devs, half_steps = topo
    ring_len = num_devs // 2
    me = lax.axis_index(axis)
    ring_pos = me // 2
    core = me % 2
    up_dev = ((ring_pos + 1) % ring_len) * 2 + core
    down_dev = ((ring_pos + ring_len - 1) % ring_len) * 2 + core
    pair_dev = ring_pos * 2 + (1 - core)
    ring_dev = (up_dev, down_dev)
    rows, width = u_ref.shape
    half_rows = rows // 2
    local_experts, _, ff_dim = eg_hbm.shape
    k_chunk = gu_buf.shape[1]
    num_k = width // k_chunk
    num_gu = local_experts * num_k
    gu_slots = gu_buf.shape[0]
    col_chunk = dn_buf.shape[2]
    num_cols = width // col_chunk
    num_dn = num_cols * local_experts
    dn_slots = dn_buf.shape[0]
    slots = x_buf.shape[1] // local_experts
    num_shared_gu = 2 * num_k
    num_shared_dn = 2 * num_cols
    half_width = width // 2
    num_pieces = 4 * half_steps - 2

    def gu_copies(j):
        slot = lax.rem(j, gu_slots)
        e = lax.div(j, num_k)
        off = pl.multiple_of(lax.rem(j, num_k) * k_chunk, k_chunk)
        return (
            pltpu.make_async_copy(eg_hbm.at[e, pl.ds(off, k_chunk), :], gu_buf.at[slot, :, pl.ds(0, ff_dim)], gu_sem.at[slot, 0]),
            pltpu.make_async_copy(eu_hbm.at[e, pl.ds(off, k_chunk), :], gu_buf.at[slot, :, pl.ds(ff_dim, ff_dim)], gu_sem.at[slot, 1]),
        )

    def shared_gu_copy(j):
        src = (sg_hbm, su_hbm)[j // num_k]
        slot = (num_gu + j) % gu_slots
        return pltpu.make_async_copy(src.at[pl.ds((j % num_k) * k_chunk, k_chunk), :], gu_buf.at[slot], gu_sem.at[slot, 0])

    def shared_dn_copy(q):
        slot = (num_dn + q) % dn_slots
        rws = pl.ds((q % 2) * ff_dim, ff_dim)
        return pltpu.make_async_copy(sd_hbm.at[rws, pl.ds((q // 2) * col_chunk, col_chunk)], dn_buf.at[slot], dn_sem.at[slot])

    def dn_copy(q):
        slot = lax.rem(q, dn_slots)
        e = lax.rem(q, local_experts)
        off = pl.multiple_of(lax.div(q, local_experts) * col_chunk, col_chunk)
        return pltpu.make_async_copy(ed_hbm.at[e, :, pl.ds(off, col_chunk)], dn_buf.at[slot], dn_sem.at[slot])

    def start_all(copies):
        for cp in copies:
            cp.start()

    def wait_all(copies):
        for cp in copies:
            cp.wait()

    for j in range(gu_slots):
        start_all(gu_copies(j))
    for q in range(dn_slots):
        dn_copy(q).start()

    barrier = pltpu.get_barrier_semaphore()
    for dev in (up_dev, down_dev, pair_dev):
        pl.semaphore_signal(barrier, inc=1, device_id={axis: dev}, device_id_type=MESH)

    num_experts = wr_ref.shape[0]
    gate_t[...] = jnp.full(gate_t.shape, -1.0, jnp.float32)
    for half in range(2):
        rws = slice(half * half_rows, (half + 1) * half_rows)
        logits = lax.dot_general(wr_ref[...], u_ref[rws], (((1,), (1,)), ((), ())), preferred_element_type=jnp.float32)
        top = jnp.max(logits, axis=0, keepdims=True)
        e_log = jnp.exp(logits - top)
        probs = e_log / jnp.sum(e_log, axis=0, keepdims=True)
        expert = lax.broadcasted_iota(jnp.int32, logits.shape, 0)
        ids = ids_ref[:, rws]
        picked = expert == ids[0:1, :]
        for k in range(1, ids.shape[0]):
            picked = picked | (expert == ids[k:k + 1, :])
        gate_t[half * num_experts:(half + 1) * num_experts, :half_rows] = jnp.where(picked, probs, -1.0)
    g_ref[...] = gate_t[...].T[:half_rows]
    pl.semaphore_wait(barrier, 3)

    def piece_part(direction, p):
        half = p % 4 // 2 if direction == 0 else 1 - p % 4 // 2
        return pl.ds(half * half_rows, half_rows), pl.ds(p % 2 * half_width, half_width)

    def held_slot(direction, step):
        return (ring_len - step) % ring_len if direction == 0 else step

    def gather_copy(direction, p):
        step = p // 4
        part_of = piece_part(direction, p)
        u_src = u_ref.at[part_of] if step == 0 else u_all.at[(0, held_slot(direction, step)) + part_of]
        return pltpu.make_async_remote_copy(src_ref=u_src, dst_ref=u_all.at[(0, held_slot(direction, step + 1)) + part_of], send_sem=agu_send.at[direction, p], recv_sem=agu_recv.at[direction, p], device_id={axis: ring_dev[direction]}, device_id_type=MESH)

    def gate_copy(direction, step):
        g_src = g_ref if step == 0 else g_all.at[0, held_slot(direction, step)]
        return pltpu.make_async_remote_copy(src_ref=g_src, dst_ref=g_all.at[0, held_slot(direction, step + 1)], send_sem=agg_send.at[direction, step], recv_sem=agg_recv.at[direction, step], device_id={axis: ring_dev[direction]}, device_id_type=MESH)

    def pair_copy(direction, p):
        piece = (held_slot(direction, p // 4 + 1),) + piece_part(direction, p)
        return pltpu.make_async_remote_copy(src_ref=u_all.at[(0,) + piece], dst_ref=u_all.at[(1,) + piece], send_sem=pru_send.at[direction, p], recv_sem=pru_recv.at[direction, p], device_id={axis: pair_dev}, device_id_type=MESH)

    def pair_gate_copy(direction, step):
        slot = held_slot(direction, step + 1)
        return pltpu.make_async_remote_copy(src_ref=g_all.at[0, slot], dst_ref=g_all.at[1, slot], send_sem=prg_send.at[direction, step], recv_sem=prg_recv.at[direction, step], device_id={axis: pair_dev}, device_id_type=MESH)

    pair_own = (
        pltpu.make_async_remote_copy(src_ref=u_ref, dst_ref=u_all.at[1, 0], send_sem=pru_send.at[0, num_pieces], recv_sem=pru_recv.at[0, num_pieces], device_id={axis: pair_dev}, device_id_type=MESH),
        pltpu.make_async_remote_copy(src_ref=g_ref, dst_ref=g_all.at[1, 0], send_sem=prg_send.at[0, half_steps], recv_sem=prg_recv.at[0, half_steps], device_id={axis: pair_dev}, device_id_type=MESH),
    )
    gate_steps = (half_steps, half_steps - 1)

    for p in range(4):
        for direction in range(2):
            if p == 0:
                gate_copy(direction, 0).start()
            gather_copy(direction, p).start()
    start_all(pair_own)
    u_all[0, 0] = u_ref[...]
    g_all[0, 0] = g_ref[...]

    for p in range(num_pieces):
        for direction in range(2):
            step = p // 4
            if p % 4 == 0 and step < gate_steps[direction]:
                gate_copy(direction, step).wait_recv()
                if step + 1 < gate_steps[direction]:
                    gate_copy(direction, step + 1).start()
                pair_gate_copy(direction, step).start()
            gather_copy(direction, p).wait_recv()
            if p + 4 < num_pieces:
                gather_copy(direction, p + 4).start()
            pair_copy(direction, p).start()
    for direction in range(2):
        for step in range(gate_steps[direction]):
            pair_gate_copy(direction, step).wait_recv()
    pair_own[1].wait_recv()

    total_rows = num_devs * rows
    lanes = g_all.shape[3]
    packed = g_all[...].reshape(total_rows // 2, lanes)
    low_half = lax.broadcasted_iota(jnp.int32, packed.shape, 1) < lanes // 2
    halves = [jnp.where(low_half, rows_of, -1.0).reshape(num_devs, half_rows, lanes) for rows_of in (packed, pltpu.roll(packed, lanes // 2, 1))]
    g_full = jnp.concatenate(halves, axis=1).reshape(total_rows, lanes)
    g_mine = pltpu.roll(g_full, lax.rem(lanes - me * local_experts, lanes), 1)
    g_loc[...] = jnp.maximum(g_mine, 0.0)
    hit = g_mine >= 0.0
    row_i = lax.broadcasted_iota(jnp.int32, (total_rows, total_rows), 0)
    col_i = lax.broadcasted_iota(jnp.int32, (total_rows, total_rows), 1)
    before = jnp.where(col_i < row_i, 1.0, 0.0).astype(jnp.bfloat16)
    rank = jnp.dot(before, jnp.where(hit, 1.0, 0.0).astype(jnp.bfloat16), preferred_element_type=jnp.float32)
    place = jnp.where(hit, rank, -1.0)
    slot_i = lax.broadcasted_iota(jnp.int32, (total_rows, slots), 1).astype(jnp.float32)
    picks = []
    for e in range(local_experts):
        one_hot = jnp.where(slot_i == place[:, e:e + 1], 1.0, 0.0)
        oht_buf[e] = one_hot.astype(jnp.bfloat16)
        picks.append(one_hot.T.astype(jnp.bfloat16))
    for direction in range(2):
        for p in range(num_pieces):
            pair_copy(direction, p).wait_recv()
    pair_own[0].wait_recv()
    u_rows = u_all[...].reshape(total_rows, width)
    for e in range(local_experts):
        for k in range(num_k):
            x_buf[k, e * slots:(e + 1) * slots] = jnp.dot(picks[e], u_rows[:, k * k_chunk:(k + 1) * k_chunk], preferred_element_type=jnp.float32).astype(jnp.bfloat16)

    def expert_step(e, carry):
        for k in range(num_k):
            j = e * num_k + k
            slot = lax.rem(j, gu_slots)
            wait_all(gu_copies(j))
            prod = jnp.dot(x_buf[k, pl.ds(pl.multiple_of(e * slots, slots), slots)], gu_buf[slot], preferred_element_type=jnp.float32)
            if k == 0:
                acc_buf[...] = prod
            else:
                acc_buf[...] += prod

            @pl.when(j + gu_slots < num_gu)
            def _():
                start_all(gu_copies(j + gu_slots))

        mid_buf[e] = (jax.nn.silu(acc_buf[:, :ff_dim]) * acc_buf[:, ff_dim:]).astype(jnp.bfloat16)
        return carry

    lax.fori_loop(0, local_experts, expert_step, 0)
    half_cols = col_chunk // 2

    pair_groups = ((half_steps - 1, 3), (0, half_steps - 1), (half_steps + 2, ring_len - half_steps - 2))

    def pair_sum_copy(c, group):
        first, count = pair_groups[group]
        span = pl.ds(first, count)
        return pltpu.make_async_remote_copy(src_ref=part.at[c, 1, span], dst_ref=px.at[c, span], send_sem=px_send.at[c, group], recv_sem=px_recv.at[c, group], device_id={axis: pair_dev}, device_id_type=MESH)

    def sum_slot(direction, step):
        return half_steps - step if direction == 0 else (half_steps + step) % ring_len

    def ring_copy(c, direction, step):
        slot = sum_slot(direction, step)
        if step == 0:
            cols = pl.ds(direction * half_cols, half_cols)
            src, dst = part.at[c, 0, slot, :, cols], ring_in.at[direction, c, step, :, cols]
        else:
            src, dst = part.at[c, 0, slot], ring_in.at[direction, c, step]
        return pltpu.make_async_remote_copy(src_ref=src, dst_ref=dst, send_sem=rs_send.at[direction, c, step], recv_sem=rs_recv.at[direction, c, step], device_id={axis: ring_dev[direction]}, device_id_type=MESH)

    def column_sums(c):
        for e in range(local_experts):
            q = c * local_experts + e
            dn_copy(q).wait()
            y_buf[e] = jnp.dot(mid_buf[e], dn_buf[q % dn_slots], preferred_element_type=jnp.float32).astype(jnp.bfloat16)
            ahead = q + dn_slots
            if ahead < num_dn:
                dn_copy(ahead).start()
            elif ahead - num_dn < num_shared_dn:
                shared_dn_copy(ahead - num_dn).start()
        for j in range(c * num_shared_gu // num_cols, (c + 1) * num_shared_gu // num_cols):
            shared_gu_copy(j).start()
        if c >= 1:
            ring_step(c - 1, 0)
        total = None
        for e in range(local_experts):
            spread = jnp.dot(oht_buf[e], y_buf[e], preferred_element_type=jnp.float32) * g_loc[:, e:e + 1]
            total = spread if total is None else total + spread
        part[c] = total.reshape(2, ring_len, rows, col_chunk)
        for group in range(len(pair_groups)):
            pair_sum_copy(c, group).start()

    def ring_step(c, step):
        if step == 0:
            pair_sum_copy(c, 0).wait_recv()
            part[c, 0, half_steps] += px[c, half_steps]
            for direction in range(2):
                ring_copy(c, direction, 0).start()
            return
        if step == 2:
            pair_sum_copy(c, 1).wait_recv()
            pair_sum_copy(c, 2).wait_recv()
        for direction in range(2):
            slot = sum_slot(direction, step)
            ring_copy(c, direction, step - 1).wait_recv()
            if step == 1:
                cols = slice(direction * half_cols, (direction + 1) * half_cols)
                part[c, 0, slot] += px[c, slot]
                part[c, 0, slot, :, cols] += ring_in[direction, c, 0, :, cols]
            elif step < half_steps:
                part[c, 0, slot] += px[c, slot] + ring_in[direction, c, step - 1]
            if step < half_steps:
                ring_copy(c, direction, step).start()
        if step == half_steps:
            part[c, 0, 0] += px[c, 0] + ring_in[0, c, step - 1] + ring_in[1, c, step - 1]

    def shared_gu(j):
        shared_gu_copy(j).wait()
        k = j % num_k
        rws = pl.ds((j // num_k) * rows, rows)
        prod = jnp.dot(u_ref[:, k * k_chunk:(k + 1) * k_chunk], gu_buf[(num_gu + j) % gu_slots], preferred_element_type=jnp.float32)
        if k == 0:
            acc_buf[rws] = prod
        else:
            acc_buf[rws] += prod
        if j == num_shared_gu - 1:
            act = (jax.nn.silu(acc_buf[:rows]) * acc_buf[rows:2 * rows]).astype(jnp.bfloat16)
            for h in range(2):
                shared_mid[h] = act[:, h * ff_dim:(h + 1) * ff_dim]

    def shared_dn(q):
        shared_dn_copy(q).wait()
        cols = slice((q // 2) * col_chunk, (q // 2 + 1) * col_chunk)
        prod = jnp.dot(shared_mid[q % 2], dn_buf[(num_dn + q) % dn_slots], preferred_element_type=jnp.float32)
        if q % 2 == 0:
            s_acc[:, cols] = prod
        else:
            s_acc[:, cols] += prod

    fillers = [functools.partial(shared_gu, j) for j in range(num_shared_gu)] + [functools.partial(shared_dn, q) for q in range(num_shared_dn)]

    for turn in range(num_cols + half_steps + 1):
        if turn < num_cols:
            column_sums(turn)
        for step in range(half_steps + 1):
            c = turn - 1 - step
            if 0 <= c < num_cols:
                if step > 0 or turn >= num_cols:
                    ring_step(c, step)
                run = 2 if turn >= num_cols else 0
                for filler in fillers[:run]:
                    filler()
                fillers = fillers[run:]
    for filler in fillers:
        filler()
    for c in range(num_cols):
        cols = slice(c * col_chunk, (c + 1) * col_chunk)
        out_ref[:, cols] = (a_ref[:, cols].astype(jnp.float32) + s_acc[:, cols] + part[c, 0, 0]).astype(jnp.bfloat16)

    for direction in range(2):
        for p in range(num_pieces):
            gather_copy(direction, p).wait_send()
            pair_copy(direction, p).wait_send()
        for step in range(gate_steps[direction]):
            gate_copy(direction, step).wait_send()
            pair_gate_copy(direction, step).wait_send()
        for c in range(num_cols):
            for step in range(half_steps):
                ring_copy(c, direction, step).wait_send()
    for cp in pair_own:
        cp.wait_send()
    for c in range(num_cols):
        for group in range(len(pair_groups)):
            pair_sum_copy(c, group).wait_send()


def moe_call(axis, num_devs, moe_in, resid_out, w_router, expert_ids, shared_gate, shared_up, shared_down, expert_gate, expert_up, expert_down, slots):
    rows, width = moe_in.shape
    local_experts, _, ff_dim = expert_gate.shape
    assert shared_down.shape[0] == 2 * ff_dim
    ring_len = num_devs // 2
    half_steps = ring_len // 2
    k_chunk = min(512, width // 2)
    num_k = width // k_chunk
    gu_slots = min(10, local_experts * num_k)
    num_cols = 4
    col_chunk = width // num_cols
    dn_slots = 10
    num_pieces = 4 * half_steps - 2
    lanes = 2 * w_router.shape[1]
    f32, bf16 = jnp.float32, jnp.bfloat16
    vmem = pl.BlockSpec(memory_space=pltpu.VMEM)
    anym = pl.BlockSpec(memory_space=pl.ANY)
    dma = pltpu.SemaphoreType.DMA
    return pl.pallas_call(
        functools.partial(moe_kernel, axis, (num_devs, half_steps)),
        name='moe_ring',
        out_shape=jax.ShapeDtypeStruct((rows, width), bf16),
        in_specs=[vmem] * 4 + [anym] * 6,
        out_specs=vmem,
        scratch_shapes=[
            pltpu.VMEM((lanes, 128), f32),
            pltpu.VMEM((rows // 2, lanes), f32),
            pltpu.VMEM((2, ring_len, rows, width), bf16),
            pltpu.VMEM((2, ring_len, rows // 2, lanes), f32),
            pltpu.VMEM((num_k, local_experts * slots, k_chunk), bf16),
            pltpu.VMEM((local_experts, num_devs * rows, slots), bf16),
            pltpu.VMEM((num_devs * rows, lanes), f32),
            pltpu.VMEM((slots, 2 * ff_dim), f32),
            pltpu.VMEM((local_experts, slots, ff_dim), bf16),
            pltpu.VMEM((2, rows, ff_dim), bf16),
            pltpu.VMEM((local_experts, slots, col_chunk), bf16),
            pltpu.VMEM((rows, width), f32),
            pltpu.VMEM((num_cols, 2, ring_len, rows, col_chunk), f32),
            pltpu.VMEM((num_cols, ring_len, rows, col_chunk), f32),
            pltpu.VMEM((2, num_cols, half_steps, rows, col_chunk), f32),
            pltpu.VMEM((gu_slots, k_chunk, 2 * ff_dim), bf16),
            pltpu.VMEM((dn_slots, ff_dim, col_chunk), bf16),
            dma((gu_slots, 2)), dma((dn_slots,)),
            dma((2, num_pieces)), dma((2, num_pieces)), dma((2, half_steps)), dma((2, half_steps)),
            dma((2, num_pieces + 1)), dma((2, num_pieces + 1)), dma((2, half_steps + 1)), dma((2, half_steps + 1)),
            dma((num_cols, 3)), dma((num_cols, 3)), dma((2, num_cols, half_steps)), dma((2, num_cols, half_steps)),
        ],
        compiler_params=pltpu.CompilerParams(collective_id=0, has_side_effects=True, vmem_limit_bytes=67043328),
    )(moe_in, resid_out, w_router.T, expert_ids.T, shared_gate, shared_up, shared_down, expert_gate, expert_up, expert_down)


def solution(mesh):
    row_spec = P(('rep', 'dp'))
    full_spec = P()
    expert_spec = P('dp')
    num_devs = mesh.shape['dp']

    def device_step(hidden, ckv_cache, kr_cache, seq_lens, expert_ids, attn_gain, kv_gain, moe_gain, w_q, w_dkv, w_uk, w_uv, w_o, w_router, shared_gate, shared_up, shared_down, expert_gate, expert_up, expert_down):
        capacity = max(2, 2 * hidden.shape[0] * expert_ids.shape[1] // w_router.shape[1])
        slots = -(-capacity * num_devs // 128) * 128
        resid_out, moe_in, ckv_new, kr_new = attn_call(hidden, ckv_cache, kr_cache, seq_lens, attn_gain, kv_gain, moe_gain, w_q, w_dkv, w_uk, w_uv, w_o)
        layer_out = moe_call('dp', num_devs, moe_in, resid_out, w_router, expert_ids, shared_gate, shared_up, shared_down, expert_gate, expert_up, expert_down, slots)
        return layer_out, ckv_new, kr_new

    in_specs = (row_spec,) * 5 + (full_spec,) * 12 + (expert_spec,) * 3
    return jax.shard_map(device_step, mesh=mesh, in_specs=in_specs, out_specs=(row_spec, row_spec, row_spec), check_vma=False)
```
